128 devices in a mesh: dom: 128 (over z, x, y, core).
Axes of the slice: x: 4, y: 4, z: 4, core: 2. Of those that a mesh axis runs over, the one named last changes fastest.
Arguments:
- features: bfloat16 [2097152, 256], P('dom'), may hold values from -48 to 48, as said below
- w_first: bfloat16 [1280, 256], replicated, may hold values from -0.15625 to 0.15625
- w_second: bfloat16 [1280, 256], replicated, may hold values from -0.15625 to 0.15625
- seed_owner: int32 [36864, 1], P('dom'), may hold values from 0 to 127; in each aligned block of 288 rows (0 to 287, 288 to 575, ...) at most 5 rows name the same one
- seed_row: int32 [36864], P('dom'), may hold values from 0 to 16383
- hop1_owner: int32 [147456, 1], P('dom'), may hold values from 0 to 127; in each aligned block of 1152 rows (0 to 1151, 1152 to 2303, ...) at most 18 rows name the same one
- hop1_row: int32 [147456], P('dom'), may hold values from 0 to 16383
- hop1_rel: int32 [147456], P('dom'), may hold values from 0 to 3
- hop2_owner: int32 [294912, 1], P('dom'), may hold values from 0 to 127; in each aligned block of 2304 rows (0 to 2303, 2304 to 4607, ...) at most 36 rows name the same one
- hop2_row: int32 [294912], P('dom'), may hold values from 0 to 16383
- hop2_rel: int32 [294912], P('dom'), may hold values from 0 to 3
- edge_mask: int32 [16384], P('dom'), may hold values 0 or 1
Outputs:
- edge_loss: float32 [16384], P('dom')
- mean_loss: float32 [], replicated
The draws below stay inside these ranges and needn't reach their ends.
Inputs may be any that keep to these rules, and one draw needn't show every extreme that they name: `features`: standard normal entries; in some draws each row is scaled by a factor up to 10. `seed_owner`: among the rows of one device no owner is named by more than 5 rows; some owner is named by exactly 5 in every draw. `hop1_owner`: among the rows of one device no owner is named by more than 18 rows; some owner is named by exactly 18 in every draw. `hop2_owner`: among the rows of one device no owner is named by more than 36 rows; some owner is named by exactly 36 in every draw.
All inputs are finite; a program needn't handle non-finite values. No bound on the sum of `edge_mask` on one device may be relied on, other than what follows from the above.
Results may differ from the reference program's by a relative error of at most 0.002.
Values may be sent and summed in bfloat16 or wider, within the bound.
A program may use at most 64 MiB of HBM per device.

```python
import math
import jax
import jax.numpy as jnp
import numpy as np
from jax import lax

F = 256
R = 4
NODE_DEV = 16384
POS_DEV = 128
BLOCK = 128
NEG = 32
FAN1 = 4
FAN2 = 2
BLOCKS_DEV = 1
SEED_DEV = 288
H1_DEV = 1152
H2_DEV = 2304
CAP_S = 5
CAP_1 = 18
CAP_2 = 36
NODES = 2097152
EDGES = 16384
SEEDS = 36864
H1 = 147456
H2 = 294912
N_DOM = 128


def draw_features(key, part):
    first_key = jax.random.fold_in(key, 0)
    values = jax.random.normal(first_key, (NODES, F), jnp.float32)
    values = jnp.clip(values, -6.0, 6.0)
    return values.astype(jnp.bfloat16)


def place_ends(array, rng, low, high):
    longest = array.shape.index(max(array.shape))
    spots = []
    for shift in (0, 1):
        where = [jax.random.randint(jax.random.fold_in(rng, axis), (), 0, length) for axis, length in enumerate(array.shape)]
        where[longest] = (where[longest] + shift) % array.shape[longest]
        spots.append(tuple(where))
    return array.at[spots[0]].set(low).at[spots[1]].set(high)


def shared_out(rng, own, number, rows, number_of, top, bound, skew):
    sequence = jax.random.permutation(rng, number_of)
    heavy_load, common = portions_of(number_of, rows * top, bound, skew, True), portions_of(number_of, rows * top, bound, skew, False)
    places = jnp.arange(number_of)

    def named(sizes, turn):
        used = int((sizes > 0).sum())
        fixed = max(1, used // 4)
        shifted = fixed + (places - fixed + turn * (used - fixed)) % max(1, number_of - fixed)
        return jnp.zeros((number_of,), jnp.int32).at[sequence[jnp.where(places < fixed, places, shifted)]].set(jnp.asarray(sizes, jnp.int32))

    sizes = jnp.where(number % 4 == 0, named(heavy_load, number // 4), named(common, number - number // 4 - 1))
    mixed = jax.random.permutation(jax.random.fold_in(own, 3), number_of)
    donor, taker = mixed[0:number_of // 2 * 2:2], mixed[1:number_of // 2 * 2:2]
    slack = jnp.minimum(sizes[donor] - 1, bound - sizes[taker]) // 2
    slack = jnp.where((donor == sequence[0]) | (taker == sequence[0]) | (sizes[taker] == 0), 0, jnp.maximum(slack, 0))
    shifted = jax.random.randint(jax.random.fold_in(own, 4), (number_of // 2,), 0, 1 << 20) % (slack + 1)
    sizes = sizes.at[donor].add(-shifted).at[taker].add(shifted)
    members = jnp.searchsorted(jnp.cumsum(sizes), jnp.arange(rows * top), side="right").astype(jnp.int32)
    grid = members.reshape(top, rows).T
    grid = grid[jax.random.permutation(jax.random.fold_in(own, 1), rows)]
    turn = jax.random.randint(jax.random.fold_in(own, 2), (rows, 1), 0, top)
    return jnp.take_along_axis(grid, (jnp.arange(top)[None, :] + turn) % top, axis=1)


def portions_of(amount, total, reach, lean, full):
    loads = [(1 << 20) // math.isqrt(standing ** lean) + 1 for standing in range(1, amount + 1)]
    largest = reach if full else min(reach, max(-(-total // amount), total * loads[0] // sum(loads)))
    least = 1 if total - largest >= amount - 1 else 0
    given, spare = [largest] + [least] * (amount - 1), total - largest - least * (amount - 1)
    while spare > 0:
        movable = [i for i in range(1, amount) if given[i] < largest] or [i for i in range(1, amount) if given[i] < reach]
        mass, remaining = sum([loads[i] for i in movable]), spare
        for i in movable:
            more = min(reach - given[i], max(1, remaining * loads[i] // mass), spare)
            given[i] = given[i] + more
            spare = spare - more
    return np.array(given)


def noise(rng, extent, scale, most, held_as=jnp.bfloat16):
    return jnp.clip(scale * jax.random.normal(rng, extent, jnp.float32), -most, most).astype(held_as)


def setup_inputs(seed: int = 0) -> dict:
    splits = jax.random.split(jax.random.key(seed), 13)
    features = draw_features(jax.random.fold_in(splits[12], 71), 0)
    w_first = noise(splits[1], ((R + 1) * F, F), ((R + 1) * F) ** -0.5, 0.15625)
    w_second = noise(splits[2], ((R + 1) * F, F), ((R + 1) * F) ** -0.5, 0.15625)
    seed_owner_keys = jax.random.split(jax.random.fold_in(splits[3], 1), SEEDS // SEED_DEV)
    seed_owner_turns = jax.random.permutation(jax.random.fold_in(splits[3], 3), SEEDS // SEED_DEV)
    seed_owner = jax.vmap(lambda own, number: shared_out(jax.random.fold_in(splits[3], 2), own, number, SEED_DEV, N_DOM, 1, CAP_S, 2))(seed_owner_keys, seed_owner_turns).reshape((SEEDS, 1))
    seed_row = place_ends(jax.random.randint(splits[4], (SEEDS,), 0, NODE_DEV), jax.random.fold_in(splits[4], 1), 0, NODE_DEV - 1).astype(jnp.int32)
    hop1_owner_keys = jax.random.split(jax.random.fold_in(splits[5], 1), H1 // H1_DEV)
    hop1_owner_turns = jax.random.permutation(jax.random.fold_in(splits[5], 3), H1 // H1_DEV)
    hop1_owner = jax.vmap(lambda own, number: shared_out(jax.random.fold_in(splits[5], 2), own, number, H1_DEV, N_DOM, 1, CAP_1, 2))(hop1_owner_keys, hop1_owner_turns).reshape((H1, 1))
    hop1_row = place_ends(jax.random.randint(splits[6], (H1,), 0, NODE_DEV), jax.random.fold_in(splits[6], 1), 0, NODE_DEV - 1).astype(jnp.int32)
    hop1_rel = place_ends(jax.random.randint(splits[7], (H1,), 0, R), jax.random.fold_in(splits[7], 1), 0, R - 1).astype(jnp.int32)
    hop2_owner_keys = jax.random.split(jax.random.fold_in(splits[8], 1), H2 // H2_DEV)
    hop2_owner_turns = jax.random.permutation(jax.random.fold_in(splits[8], 3), H2 // H2_DEV)
    hop2_owner = jax.vmap(lambda own, number: shared_out(jax.random.fold_in(splits[8], 2), own, number, H2_DEV, N_DOM, 1, CAP_2, 2))(hop2_owner_keys, hop2_owner_turns).reshape((H2, 1))
    hop2_row = place_ends(jax.random.randint(splits[9], (H2,), 0, NODE_DEV), jax.random.fold_in(splits[9], 1), 0, NODE_DEV - 1).astype(jnp.int32)
    hop2_rel = place_ends(jax.random.randint(splits[10], (H2,), 0, R), jax.random.fold_in(splits[10], 1), 0, R - 1).astype(jnp.int32)
    edge_mask = place_ends((jax.random.randint(splits[11], (EDGES,), 0, 4) < 3).astype(jnp.int32), jax.random.fold_in(splits[11], 1), 0, 1)
    return dict(features=features, w_first=w_first, w_second=w_second, seed_owner=seed_owner, seed_row=seed_row, hop1_owner=hop1_owner, hop1_row=hop1_row, hop1_rel=hop1_rel, hop2_owner=hop2_owner, hop2_row=hop2_row, hop2_rel=hop2_rel, edge_mask=edge_mask)


def rgcn_layer(self_rows, neighbours, relations, weights):
    onehot = (relations[..., None] == jnp.arange(R, dtype=jnp.int32)).astype(jnp.float32)
    tallies = jnp.maximum(jnp.sum(onehot, axis=1), 1.0)
    shares = onehot / tallies[:, None, :]
    merged = jnp.einsum('nkr,nkf->nrf', shares, neighbours.astype(jnp.float32)).astype(jnp.bfloat16)
    inputs = jnp.concatenate([self_rows, merged.reshape(self_rows.shape[0], R * F)], axis=1)
    return jnp.dot(inputs, weights, preferred_element_type=jnp.float32)


def edge_scores(second):
    sources = second[:POS_DEV]
    targets = second[POS_DEV:2 * POS_DEV]
    negatives = second[2 * POS_DEV:].reshape(BLOCKS_DEV, NEG, F)
    positive = jnp.sum(sources * targets, axis=1)
    negative = jnp.einsum('bef,bqf->beq', sources.reshape(BLOCKS_DEV, BLOCK, F), negatives,
                          precision=lax.Precision.HIGHEST).reshape(POS_DEV, NEG)
    scores = jnp.concatenate([positive[:, None], negative], axis=1)
    top_score = jnp.max(scores, axis=1, keepdims=True)
    return top_score[:, 0] + jnp.log(jnp.sum(jnp.exp(scores - top_score), axis=1)) - positive


def reference(features, w_first, w_second, seed_owner, seed_row, hop1_owner, hop1_row, hop1_rel,
              hop2_owner, hop2_row, hop2_rel, edge_mask):
    def one_device(pieces):
        s_owner, s_row, a_owner, a_row, a_rel, b_owner, b_row, b_rel = pieces
        x_seed = features[(s_owner * NODE_DEV + s_row).astype(jnp.int32)]
        x_hop1 = features[(a_owner * NODE_DEV + a_row).astype(jnp.int32)]
        x_hop2 = features[(b_owner * NODE_DEV + b_row).astype(jnp.int32)]
        first_hop = jax.nn.relu(rgcn_layer(x_hop1, x_hop2.reshape(H1_DEV, FAN2, F),
                                           b_rel.reshape(H1_DEV, FAN2), w_first)).astype(jnp.bfloat16)
        first_seed = jax.nn.relu(rgcn_layer(x_seed, x_hop1.reshape(SEED_DEV, FAN1, F),
                                            a_rel.reshape(SEED_DEV, FAN1), w_first)).astype(jnp.bfloat16)
        second = rgcn_layer(first_seed, first_hop.reshape(SEED_DEV, FAN1, F),
                            a_rel.reshape(SEED_DEV, FAN1), w_second)
        return edge_scores(second)

    pieces = (seed_owner.reshape(N_DOM, SEED_DEV), seed_row.reshape(N_DOM, SEED_DEV),
              hop1_owner.reshape(N_DOM, H1_DEV), hop1_row.reshape(N_DOM, H1_DEV),
              hop1_rel.reshape(N_DOM, H1_DEV), hop2_owner.reshape(N_DOM, H2_DEV),
              hop2_row.reshape(N_DOM, H2_DEV), hop2_rel.reshape(N_DOM, H2_DEV))
    edge_loss = lax.map(one_device, pieces).reshape(EDGES)
    weights = edge_mask.astype(jnp.float32)
    mean_loss = jnp.sum(weights * edge_loss) / jnp.maximum(jnp.sum(weights), 1.0)
    return edge_loss, mean_loss
```

```python
import functools

import jax
import jax.numpy as jnp
from jax import lax
from jax.experimental import pallas as pl
from jax.experimental.pallas import tpu as pltpu
from jax.sharding import PartitionSpec as P

R = 4
FAN1 = 4
FAN2 = 2
LANES = 128
STEP = 45
LOGICAL = pl.DeviceIdType.LOGICAL
F32 = jnp.float32
BF16 = jnp.bfloat16
NT = (((1,), (1,)), ((), ()))


def kernel(
    n, count, caps,
    feat_hbm, wf_hbm, ws_hbm,
    own0_hbm, row0_hbm, own1_hbm, row1_hbm, rel1_hbm, own2_hbm, row2_hbm, rel2_hbm, mask_hbm,
    loss_ref, mean_ref,
    own0, row0, own1, row1, rel1, own2, row2, rel2, mask_ref,
    fbf, fsp, wf, ws, pad_own, pad_row, slots0, slots1, slots2, req_out, req_in,
    send0, send1, send2, recv0, recv1, recv2, x0, x1, x2, min1, min0, h1l, h1r, relc1, relc2,
    part_out, part_in,
    req_s, slot0_s, slot1_s, slot2_s,
    isem, fsem, wsem, qsend, qrecv, ssem, rsem, tsem, psend, precv,
):
    n_seed, n_one, n_two = count
    cap0, cap1, cap2 = caps
    bases = (0, cap0, cap0 + cap1)
    me = lax.axis_index("dom")
    width = wf.shape[1]
    nodes = fbf.shape[0]
    gap = fsp.shape[0] - nodes

    def target(k):
        return lax.rem(me + lax.rem(k * STEP, n), n)

    here_refs = (own2, row2, own1, row1, own0, row0, rel2, rel1, mask_ref)
    there_refs = (
        own2_hbm, row2_hbm, own1_hbm, row1_hbm, own0_hbm, row0_hbm, rel2_hbm, rel1_hbm, mask_hbm
    )
    index_copies = [
        pltpu.make_async_copy(a, b if len(a.shape) == 2 else b.at[0], isem.at[i])
        for i, (a, b) in enumerate(zip(there_refs, here_refs))
    ]
    for copy in index_copies:
        copy.start()

    barrier = pltpu.get_barrier_semaphore()

    def greet(k, _):
        pl.semaphore_signal(barrier, 1, device_id=target(k), device_id_type=LOGICAL)
        return 0

    lax.fori_loop(1, n, greet, 0)
    chunks = fsem.shape[0]
    part = nodes // chunks
    feat_copies = [
        pltpu.make_async_copy(
            feat_hbm.at[pl.ds(i * part, part)], fbf.at[pl.ds(i * part, part)], fsem.at[i]
        )
        for i in range(chunks)
    ]
    for copy in feat_copies:
        copy.start()
    w_copies = [
        pltpu.make_async_copy(wf_hbm, wf, wsem.at[0]),
        pltpu.make_async_copy(ws_hbm, ws, wsem.at[1]),
    ]
    for copy in w_copies:
        copy.start()

    iota_own = lax.broadcasted_iota(jnp.int32, (n, LANES), 0)
    iota_slot = lax.broadcasted_iota(jnp.int32, (64, LANES), 0)
    upper = lax.broadcasted_iota(jnp.int32, (LANES, LANES), 0) < lax.broadcasted_iota(
        jnp.int32, (LANES, LANES), 1
    )
    ladder = jnp.concatenate(
        [jnp.where(upper, 1.0, 0.0).astype(BF16), jnp.ones((LANES, LANES), BF16)], axis=1
    )

    def bucket(owner_ref, row_ref, slots, cap, base, blocks, table):
        def block(b, carry):
            before, table = carry
            cols = pl.ds(pl.multiple_of(b * LANES, LANES), LANES)
            owner = owner_ref[:, cols]
            rows = row_ref[:, cols]
            hot = jnp.where(iota_own == owner, 1.0, 0.0)
            hot16 = hot.astype(BF16)
            counts = jnp.dot(hot16, ladder, preferred_element_type=F32)
            prior = counts[:, :LANES] + before
            place = jnp.sum(hot * prior, axis=0, keepdims=True).astype(jnp.int32)
            place = jnp.clip(place, 0, cap - 1)
            slots[:, cols] = owner * cap + place
            here = iota_slot == place + base
            high = (rows >> 7).astype(F32)
            low = (rows & 127).astype(F32)
            values = jnp.concatenate(
                [jnp.where(here, high, 0.0), jnp.where(here, low, 0.0)], axis=0
            ).astype(BF16)
            table = table + lax.dot_general(hot16, values, NT, preferred_element_type=F32)
            return before + counts[:, LANES:], table

        zero = jnp.zeros((n, LANES), F32)
        return lax.fori_loop(0, blocks, block, (zero, table))[1]

    for copy in index_copies[:6]:
        copy.wait()
    pad_own[...] = jnp.full(pad_own.shape, -1, jnp.int32)
    pad_row[...] = jnp.zeros(pad_row.shape, jnp.int32)
    pad_own[:, :n_seed] = own0[...]
    pad_row[:, :n_seed] = row0[...]
    table = jnp.zeros((n, LANES), F32)
    table = bucket(own2, row2, slots2, cap2, bases[2], n_two // LANES, table)
    table = bucket(own1, row1, slots1, cap1, bases[1], n_one // LANES, table)
    table = bucket(pad_own, pad_row, slots0, cap0, bases[0], pad_own.shape[1] // LANES, table)
    wanted = (table * 128.0 + pltpu.roll(table, 64, 1)).astype(jnp.int32)
    wanted = jnp.clip(wanted, 0, nodes - 1)
    for i in range(n):
        req_out[i] = wanted[i : i + 1]

    def widen(i, _):
        step = 128
        r = pl.multiple_of(i * step, step)
        rows = fbf[pl.ds(r, step), :].astype(F32)
        fsp[pl.ds(r, step), :] = rows[:, :LANES]
        fsp[pl.ds(pl.multiple_of(r + gap, 8), step), :] = rows[:, LANES:]
        return 0

    per_chunk = part // 128
    feat_copies[0].wait()
    lax.fori_loop(0, per_chunk, widen, 0)

    pl.semaphore_wait(barrier, n - 1)

    def ask(k, _):
        t = target(k)
        pltpu.make_async_remote_copy(
            src_ref=req_out.at[t], dst_ref=req_in.at[me], send_sem=qsend, recv_sem=qrecv,
            device_id=t, device_id_type=LOGICAL,
        ).start()
        return 0

    lax.fori_loop(1, n, ask, 0)
    req_in[me] = req_out[me]

    for i in range(1, chunks):
        feat_copies[i].wait()
        lax.fori_loop(i * per_chunk, (i + 1) * per_chunk, widen, 0)

    rest = pl.ds(0, n - 1)
    pltpu.make_async_copy(req_in.at[rest], req_in.at[rest], qrecv).wait()
    small = [
        pltpu.make_async_copy(req_in, req_s, tsem.at[0]),
        pltpu.make_async_copy(slots2, slot2_s, tsem.at[1]),
        pltpu.make_async_copy(slots1, slot1_s, tsem.at[2]),
        pltpu.make_async_copy(slots0, slot0_s, tsem.at[3]),
    ]
    for copy in small:
        copy.start()
    small[0].wait()

    hops = ((send2, recv2, cap2, bases[2], 2), (send1, recv1, cap1, bases[1], 1), (send0, recv0, cap0, bases[0], 0))

    def gather(t, out, cap, base):
        for j in range(cap):
            node = req_s[t, 0, base + j]
            pair = fsp[pl.ds(node, 2, stride=gap), :]
            out[t * cap + j] = pair.astype(BF16)

    def start_send(t, out, into, cap, h):
        pltpu.make_async_remote_copy(
            src_ref=out.at[pl.ds(t * cap, cap)], dst_ref=into.at[pl.ds(me * cap, cap)],
            send_sem=ssem.at[h], recv_sem=rsem.at[h], device_id=t, device_id_type=LOGICAL,
        ).start()

    for out, into, cap, base, h in hops:

        def serve(k, _, out=out, into=into, cap=cap, base=base, h=h):
            gather(target(k), out, cap, base)
            start_send(target(k - 1), out, into, cap, h)
            return 0

        gather(target(1), out, cap, base)
        lax.fori_loop(2, n, serve, 0)
        gather(me, into, cap, base)
        start_send(target(n - 1), out, into, cap, h)

    for copy in index_copies[6:]:
        copy.wait()

    def relation_columns(rel_ref, out, blocks):
        def block(b, _):
            at = pl.multiple_of(b * LANES, LANES)
            row = rel_ref[:, pl.ds(at, LANES)].astype(F32)
            out[pl.ds(at, LANES), :] = jnp.broadcast_to(row, (LANES, LANES)).T
            return 0

        lax.fori_loop(0, blocks, block, 0)

    relation_columns(rel2, relc2, n_two // LANES)
    relation_columns(rel1, relc1, n_one // LANES)
    for copy in small[1:]:
        copy.wait()
    for copy in w_copies:
        copy.wait()

    def unpack(slot_s, came, out, total):
        batch = 32

        def some(b, _):
            for j in range(batch):
                i = b * batch + j
                pair = came[slot_s[0, i]].astype(F32)
                out[pl.ds(pl.multiple_of(i * 2, 2), 2), :] = pair
            return 0

        lax.fori_loop(0, total // batch, some, 0)

    def arrived(h, came, cap):
        got = came.at[pl.ds(0, (n - 1) * cap)]
        pltpu.make_async_copy(got, got, rsem.at[h]).wait()

    arrived(2, recv2, cap2)
    unpack(slot2_s, recv2, x2, n_two)
    tile = 32

    def two_means(b, _):
        f = pl.multiple_of(b * tile, tile)
        ra = relc2[pl.ds(FAN2 * f, tile, stride=FAN2), :]
        rb = relc2[pl.ds(FAN2 * f + 1, tile, stride=FAN2), :]
        share = jnp.where(ra == rb, 0.5, 1.0)
        for half in range(2):
            a = x2[pl.ds(4 * f + half, tile, stride=4), :] * share
            v = x2[pl.ds(4 * f + 2 + half, tile, stride=4), :] * share
            for r in range(R):
                mean = jnp.where(ra == r, a, 0.0) + jnp.where(rb == r, v, 0.0)
                at = r * width + half * LANES
                min1[pl.ds(f, tile), at : at + LANES] = mean.astype(BF16)
        return 0

    lax.fori_loop(0, n_one // tile, two_means, 0)

    arrived(1, recv1, cap1)
    unpack(slot1_s, recv1, x1, n_one)
    rows = 128

    def first_layer(b, _):
        f = pl.multiple_of(b * rows, rows)
        own = jnp.concatenate(
            [x1[pl.ds(2 * f, rows, stride=2), :], x1[pl.ds(2 * f + 1, rows, stride=2), :]], axis=1
        ).astype(BF16)
        total = jnp.dot(own, wf[:width, :], preferred_element_type=F32)
        total = total + jnp.dot(
            min1[pl.ds(f, rows), :], wf[width:, :], preferred_element_type=F32
        )
        out = jnp.maximum(total, 0.0).astype(BF16).astype(F32)
        h1l[pl.ds(f, rows), :] = out[:, :LANES]
        h1r[pl.ds(f, rows), :] = out[:, LANES:]
        return 0

    lax.fori_loop(0, n_one // rows, first_layer, 0)

    def four_means(load):
        def some(b, _):
            s = pl.multiple_of(b * tile, tile)
            rels = [relc1[pl.ds(FAN1 * s + j, tile, stride=FAN1), :] for j in range(FAN1)]
            for r in range(R):
                hits = [rel == r for rel in rels]
                tally = sum(jnp.where(hit, 1.0, 0.0) for hit in hits)
                share = jnp.where(
                    tally == 4.0, 0.25, jnp.where(tally == 3.0, 1.0 / 3.0, jnp.where(tally == 2.0, 0.5, 1.0))
                )
                for half in range(2):
                    total = sum(
                        jnp.where(hits[j], load(s, j, half), 0.0) for j in range(FAN1)
                    )
                    at = r * width + half * LANES
                    min0[pl.ds(s, tile), at : at + LANES] = (total * share).astype(BF16)
            return 0

        lax.fori_loop(0, n_seed // tile, some, 0)

    four_means(lambda s, j, half: x1[pl.ds(8 * s + 2 * j + half, tile, stride=8), :])
    seed_part = jnp.dot(min0[...], wf[width:, :], preferred_element_type=F32)
    four_means(
        lambda s, j, half: (h1l, h1r)[half][pl.ds(FAN1 * s + j, tile, stride=FAN1), :]
    )
    second_part = jnp.dot(min0[...], ws[width:, :], preferred_element_type=F32)

    arrived(0, recv0, cap0)
    unpack(slot0_s, recv0, x0, n_seed)
    own = jnp.concatenate(
        [x0[pl.ds(0, n_seed, stride=2), :], x0[pl.ds(1, n_seed, stride=2), :]], axis=1
    ).astype(BF16)
    h1s = jnp.maximum(
        jnp.dot(own, wf[:width, :], preferred_element_type=F32) + seed_part, 0.0
    ).astype(BF16)
    second = jnp.dot(h1s, ws[:width, :], preferred_element_type=F32) + second_part

    edges = mask_ref.shape[1]
    sources = second[:edges]
    products = sources * second[edges : 2 * edges]
    positive = lax.dot_general(
        jnp.ones((8, width), F32), products, NT,
        precision=lax.Precision.HIGHEST, preferred_element_type=F32,
    )[:1]
    negative = lax.dot_general(
        second[2 * edges :], sources, NT,
        precision=lax.Precision.HIGHEST, preferred_element_type=F32,
    )
    top = jnp.maximum(jnp.max(negative, axis=0, keepdims=True), positive)
    spread = jnp.sum(jnp.exp(negative - top), axis=0, keepdims=True) + jnp.exp(positive - top)
    edge_loss = top + jnp.log(spread) - positive
    loss_ref[...] = edge_loss
    weights = mask_ref[...].astype(F32)
    both = jnp.concatenate([weights * edge_loss, weights], axis=0)
    part_out[...] = both
    part_in[me] = both

    def tell(k, _):
        pltpu.make_async_remote_copy(
            src_ref=part_out, dst_ref=part_in.at[me], send_sem=psend, recv_sem=precv,
            device_id=target(k), device_id_type=LOGICAL,
        ).start()
        return 0

    sent = req_out.at[rest]
    pltpu.make_async_copy(sent, sent, qsend).wait()
    for out, _, cap, _, h in hops:
        sent = out.at[pl.ds(0, (n - 1) * cap)]
        pltpu.make_async_copy(sent, sent, ssem.at[h]).wait()
    lax.fori_loop(1, n, tell, 0)
    told = part_in.at[rest]
    pltpu.make_async_copy(told, told, precv).wait()
    sums = jnp.sum(jnp.sum(part_in[...], axis=0), axis=1, keepdims=True)
    mean_ref[...] = jnp.broadcast_to(
        sums[:1] / jnp.maximum(sums[1:], 1.0), mean_ref.shape
    )
    pltpu.make_async_copy(told, told, psend).wait()


def solution(mesh):
    n = mesh.shape["dom"]

    def shards(
        features, w_first, w_second, seed_owner, seed_row, hop1_owner, hop1_row, hop1_rel,
        hop2_owner, hop2_row, hop2_rel, edge_mask,
    ):
        nodes, width = features.shape
        n_seed, n_one, n_two = seed_row.shape[0], hop1_row.shape[0], hop2_row.shape[0]
        edges = edge_mask.shape[0]
        caps = tuple(-(-2 * m // n) for m in (n_seed, n_one, n_two))
        cap0, cap1, cap2 = caps
        padded = -(-n_seed // LANES) * LANES
        vmem, hbm = pl.BlockSpec(memory_space=pltpu.VMEM), pl.BlockSpec(memory_space=pl.ANY)
        dma = pltpu.SemaphoreType.DMA

        def rows_of(cap):
            return pltpu.VMEM((n * cap, 2, LANES), BF16)

        def line(m):
            return pltpu.VMEM((1, m), jnp.int32)

        scratch = [
            line(n_seed), line(n_seed), line(n_one), line(n_one), line(n_one),
            line(n_two), line(n_two), line(n_two), line(edges),
            pltpu.VMEM((nodes, width), BF16),
            pltpu.VMEM((2 * nodes + 8, LANES), F32),
            pltpu.VMEM(w_first.shape, BF16),
            pltpu.VMEM(w_second.shape, BF16),
            pltpu.VMEM((1, padded), jnp.int32),
            pltpu.VMEM((1, padded), jnp.int32),
            pltpu.VMEM((1, padded), jnp.int32),
            pltpu.VMEM((1, n_one), jnp.int32),
            pltpu.VMEM((1, n_two), jnp.int32),
            pltpu.VMEM((n, 1, LANES), jnp.int32),
            pltpu.VMEM((n, 1, LANES), jnp.int32),
            rows_of(cap0), rows_of(cap1), rows_of(cap2),
            rows_of(cap0), rows_of(cap1), rows_of(cap2),
            pltpu.VMEM((2 * n_seed, LANES), F32),
            pltpu.VMEM((2 * n_one, LANES), F32),
            pltpu.VMEM((2 * n_two, LANES), F32),
            pltpu.VMEM((n_one, R * width), BF16),
            pltpu.VMEM((n_seed, R * width), BF16),
            pltpu.VMEM((n_one, LANES), F32),
            pltpu.VMEM((n_one, LANES), F32),
            pltpu.VMEM((n_one, LANES), F32),
            pltpu.VMEM((n_two, LANES), F32),
            pltpu.VMEM((2, edges), F32),
            pltpu.VMEM((n, 2, edges), F32),
            pltpu.SMEM((n, 1, LANES), jnp.int32),
            pltpu.SMEM((1, padded), jnp.int32),
            pltpu.SMEM((1, n_one), jnp.int32),
            pltpu.SMEM((1, n_two), jnp.int32),
            dma((9,)), dma((4,)), dma((2,)), dma, dma, dma((3,)), dma((3,)), dma((4,)), dma, dma,
        ]
        edge_loss, mean = pl.pallas_call(
            functools.partial(kernel, n, (n_seed, n_one, n_two), caps),
            out_shape=(
                jax.ShapeDtypeStruct((1, edges), F32),
                jax.ShapeDtypeStruct((1, LANES), F32),
            ),
            in_specs=[hbm] * 12,
            out_specs=(vmem, vmem),
            scratch_shapes=scratch,
            compiler_params=pltpu.CompilerParams(
                collective_id=0, has_side_effects=True, vmem_limit_bytes=62 * 2**20
            ),
            name="fetch_and_score",
        )(
            features, w_first, w_second,
            seed_owner.reshape(1, n_seed), seed_row,
            hop1_owner.reshape(1, n_one), hop1_row, hop1_rel,
            hop2_owner.reshape(1, n_two), hop2_row, hop2_rel, edge_mask,
        )
        return edge_loss.reshape(edges), mean[0, 0]

    dom = P("dom")
    tall = P("dom", None)
    return jax.shard_map(
        shards,
        mesh=mesh,
        in_specs=(tall, P(), P(), tall, dom, tall, dom, dom, tall, dom, dom, dom),
        out_specs=(dom, P()),
        check_vma=False,
    )
```

```python
import functools
import itertools

import jax
import jax.numpy as jnp
from jax import lax
from jax.experimental import pallas as pl
from jax.experimental.pallas import tpu as pltpu
from jax.sharding import PartitionSpec as P

R = 4
FAN1 = 4
FAN2 = 2
LANES = 128
SIDE = 4
STEP = 45
LOGICAL = pl.DeviceIdType.LOGICAL
F32 = jnp.float32
BF16 = jnp.bfloat16
NT = (((1,), (1,)), ((), ()))


def kernel(
    n, count, caps,
    feat_hbm, wf_hbm, ws_hbm,
    own0_hbm, row0_hbm, own1_hbm, row1_hbm, rel1_hbm, own2_hbm, row2_hbm, rel2_hbm, mask_hbm,
    loss_ref, mean_ref,
    own0, row0, own1, row1, rel1, own2, row2, rel2, mask_ref,
    fbf, fsp, wf, ws, pad_own, pad_row, slots0, slots1, slots2, req_out, req_in,
    send0, send1, send2, recv0, recv1, recv2, x0, x1, x2, min1, min0, h1l, h1r, relc1, relc2,
    part_out, part_in,
    req_s, slot0_s, slot1_s, slot2_s,
    isem, fsem, wsem, qsend, qrecv, ssem, rsem, tsem, psend, precv,
):
    n_seed, n_one, n_two = count
    cap0, cap1, cap2 = caps
    bases = (0, cap0, cap0 + cap1)
    me = lax.axis_index("dom")
    width = wf.shape[1]
    nodes = fbf.shape[0]
    gap = fsp.shape[0] - nodes

    def target(k):
        return lax.rem(me + lax.rem(k * STEP, n), n)

    side = SIDE
    spots = []
    scale = n
    for length in (side, side, side, 2):
        scale //= length
        at = lax.rem(lax.div(me, scale), length)
        spots.append([lax.rem(at + d, length) * scale for d in range(length)])
    offsets = sorted(
        itertools.product(range(side), range(side), range(side), range(2)),
        key=lambda o: (-sum(min(d, side - d) for d in o[:3]), o),
    )
    peers = [sum(spot[d] for spot, d in zip(spots, o)) for o in offsets if any(o)]

    here_refs = (own2, row2, own1, row1, own0, row0, rel2, rel1, mask_ref)
    there_refs = (
        own2_hbm, row2_hbm, own1_hbm, row1_hbm, own0_hbm, row0_hbm, rel2_hbm, rel1_hbm, mask_hbm
    )
    index_copies = [
        pltpu.make_async_copy(a, b if len(a.shape) == 2 else b.at[0], isem.at[i])
        for i, (a, b) in enumerate(zip(there_refs, here_refs))
    ]
    for copy in index_copies:
        copy.start()

    barrier = pltpu.get_barrier_semaphore()

    for t in peers:
        pl.semaphore_signal(barrier, 1, device_id=t, device_id_type=LOGICAL)
    chunks = fsem.shape[0]
    part = nodes // chunks
    feat_copies = [
        pltpu.make_async_copy(
            feat_hbm.at[pl.ds(i * part, part)], fbf.at[pl.ds(i * part, part)], fsem.at[i]
        )
        for i in range(chunks)
    ]
    for copy in feat_copies:
        copy.start()
    w_copies = [
        pltpu.make_async_copy(wf_hbm, wf, wsem.at[0]),
        pltpu.make_async_copy(ws_hbm, ws, wsem.at[1]),
    ]
    for copy in w_copies:
        copy.start()

    iota_own = lax.broadcasted_iota(jnp.int32, (n, LANES), 0)
    iota_slot = lax.broadcasted_iota(jnp.int32, (64, LANES), 0)
    upper = lax.broadcasted_iota(jnp.int32, (LANES, LANES), 0) < lax.broadcasted_iota(
        jnp.int32, (LANES, LANES), 1
    )
    ladder = jnp.concatenate(
        [jnp.where(upper, 1.0, 0.0).astype(BF16), jnp.ones((LANES, LANES), BF16)], axis=1
    )

    def bucket(owner_ref, row_ref, slots, cap, base, blocks, table):
        def block(b, carry):
            before, table = carry
            cols = pl.ds(pl.multiple_of(b * LANES, LANES), LANES)
            owner = owner_ref[:, cols]
            rows = row_ref[:, cols]
            hot = jnp.where(iota_own == owner, 1.0, 0.0)
            hot16 = hot.astype(BF16)
            counts = jnp.dot(hot16, ladder, preferred_element_type=F32)
            prior = counts[:, :LANES] + before
            place = jnp.sum(hot * prior, axis=0, keepdims=True).astype(jnp.int32)
            place = jnp.clip(place, 0, cap - 1)
            slots[:, cols] = owner * cap + place
            here = iota_slot == place + base
            high = (rows >> 7).astype(F32)
            low = (rows & 127).astype(F32)
            values = jnp.concatenate(
                [jnp.where(here, high, 0.0), jnp.where(here, low, 0.0)], axis=0
            ).astype(BF16)
            table = table + lax.dot_general(hot16, values, NT, preferred_element_type=F32)
            return before + counts[:, LANES:], table

        zero = jnp.zeros((n, LANES), F32)
        return lax.fori_loop(0, blocks, block, (zero, table), unroll=3)[1]

    for copy in index_copies[:6]:
        copy.wait()
    pad_own[...] = jnp.full(pad_own.shape, -1, jnp.int32)
    pad_row[...] = jnp.zeros(pad_row.shape, jnp.int32)
    pad_own[:, :n_seed] = own0[...]
    pad_row[:, :n_seed] = row0[...]
    table = jnp.zeros((n, LANES), F32)
    table = bucket(own2, row2, slots2, cap2, bases[2], n_two // LANES, table)
    table = bucket(own1, row1, slots1, cap1, bases[1], n_one // LANES, table)
    table = bucket(pad_own, pad_row, slots0, cap0, bases[0], pad_own.shape[1] // LANES, table)
    wanted = (table * 128.0 + pltpu.roll(table, 64, 1)).astype(jnp.int32)
    wanted = jnp.clip(wanted, 0, nodes - 1)
    for i in range(n):
        req_out[i] = wanted[i : i + 1]

    def widen(i, _):
        step = 128
        r = pl.multiple_of(i * step, step)
        rows = fbf[pl.ds(r, step), :].astype(F32)
        fsp[pl.ds(r, step), :] = rows[:, :LANES]
        fsp[pl.ds(pl.multiple_of(r + gap, 8), step), :] = rows[:, LANES:]
        return 0

    per_chunk = part // 128
    feat_copies[0].wait()
    lax.fori_loop(0, per_chunk, widen, 0)

    pl.semaphore_wait(barrier, n - 1)

    for t in peers:
        pltpu.make_async_remote_copy(
            src_ref=req_out.at[t], dst_ref=req_in.at[me], send_sem=qsend, recv_sem=qrecv,
            device_id=t, device_id_type=LOGICAL,
        ).start()
    req_in[me] = req_out[me]

    for i in range(1, chunks):
        feat_copies[i].wait()
        lax.fori_loop(i * per_chunk, (i + 1) * per_chunk, widen, 0)

    rest = pl.ds(0, n - 1)
    pltpu.make_async_copy(req_in.at[rest], req_in.at[rest], qrecv).wait()
    small = [
        pltpu.make_async_copy(req_in, req_s, tsem.at[0]),
        pltpu.make_async_copy(slots2, slot2_s, tsem.at[1]),
        pltpu.make_async_copy(slots1, slot1_s, tsem.at[2]),
        pltpu.make_async_copy(slots0, slot0_s, tsem.at[3]),
    ]
    for copy in small:
        copy.start()
    small[0].wait()

    hops = ((send2, recv2, cap2, bases[2], 2), (send1, recv1, cap1, bases[1], 1), (send0, recv0, cap0, bases[0], 0))

    def gather(t, out, cap, base):
        for j in range(cap):
            node = req_s[t, 0, base + j]
            pair = fsp[pl.ds(node, 2, stride=gap), :]
            out[t * cap + j] = pair.astype(BF16)

    def start_send(t, out, into, cap, h):
        pltpu.make_async_remote_copy(
            src_ref=out.at[pl.ds(t * cap, cap)], dst_ref=into.at[pl.ds(me * cap, cap)],
            send_sem=ssem.at[h], recv_sem=rsem.at[h], device_id=t, device_id_type=LOGICAL,
        ).start()

    for out, into, cap, base, h in hops:

        def serve(k, _, out=out, into=into, cap=cap, base=base, h=h):
            gather(target(k), out, cap, base)
            start_send(target(k - 1), out, into, cap, h)
            return 0

        gather(target(1), out, cap, base)
        lax.fori_loop(2, n, serve, 0)
        gather(me, into, cap, base)
        start_send(target(n - 1), out, into, cap, h)

    for copy in index_copies[6:]:
        copy.wait()

    def relation_columns(rel_ref, out, blocks):
        def block(b, _):
            at = pl.multiple_of(b * LANES, LANES)
            row = rel_ref[:, pl.ds(at, LANES)].astype(F32)
            out[pl.ds(at, LANES), :] = jnp.broadcast_to(row, (LANES, LANES)).T
            return 0

        lax.fori_loop(0, blocks, block, 0)

    relation_columns(rel2, relc2, n_two // LANES)
    relation_columns(rel1, relc1, n_one // LANES)
    for copy in small[1:]:
        copy.wait()
    for copy in w_copies:
        copy.wait()

    def unpack(slot_s, came, out, total):
        batch = 32

        def some(b, _):
            for j in range(batch):
                i = b * batch + j
                pair = came[slot_s[0, i]].astype(F32)
                out[pl.ds(pl.multiple_of(i * 2, 2), 2), :] = pair
            return 0

        lax.fori_loop(0, total // batch, some, 0)

    def arrived(h, came, cap):
        got = came.at[pl.ds(0, (n - 1) * cap)]
        pltpu.make_async_copy(got, got, rsem.at[h]).wait()

    arrived(2, recv2, cap2)
    unpack(slot2_s, recv2, x2, n_two)
    tile = 32

    def two_means(b, _):
        f = pl.multiple_of(b * tile, tile)
        ra = relc2[pl.ds(FAN2 * f, tile, stride=FAN2), :]
        rb = relc2[pl.ds(FAN2 * f + 1, tile, stride=FAN2), :]
        share = jnp.where(ra == rb, 0.5, 1.0)
        for half in range(2):
            a = x2[pl.ds(4 * f + half, tile, stride=4), :] * share
            v = x2[pl.ds(4 * f + 2 + half, tile, stride=4), :] * share
            for r in range(R):
                mean = jnp.where(ra == r, a, 0.0) + jnp.where(rb == r, v, 0.0)
                at = r * width + half * LANES
                min1[pl.ds(f, tile), at : at + LANES] = mean.astype(BF16)
        return 0

    lax.fori_loop(0, n_one // tile, two_means, 0)

    arrived(1, recv1, cap1)
    unpack(slot1_s, recv1, x1, n_one)
    rows = 128

    def first_layer(b, _):
        f = pl.multiple_of(b * rows, rows)
        own = jnp.concatenate(
            [x1[pl.ds(2 * f, rows, stride=2), :], x1[pl.ds(2 * f + 1, rows, stride=2), :]], axis=1
        ).astype(BF16)
        total = jnp.dot(own, wf[:width, :], preferred_element_type=F32)
        total = total + jnp.dot(
            min1[pl.ds(f, rows), :], wf[width:, :], preferred_element_type=F32
        )
        out = jnp.maximum(total, 0.0).astype(BF16).astype(F32)
        h1l[pl.ds(f, rows), :] = out[:, :LANES]
        h1r[pl.ds(f, rows), :] = out[:, LANES:]
        return 0

    lax.fori_loop(0, n_one // rows, first_layer, 0)

    def four_means(load):
        def some(b, _):
            s = pl.multiple_of(b * tile, tile)
            rels = [relc1[pl.ds(FAN1 * s + j, tile, stride=FAN1), :] for j in range(FAN1)]
            for r in range(R):
                hits = [rel == r for rel in rels]
                tally = sum(jnp.where(hit, 1.0, 0.0) for hit in hits)
                share = jnp.where(
                    tally == 4.0, 0.25, jnp.where(tally == 3.0, 1.0 / 3.0, jnp.where(tally == 2.0, 0.5, 1.0))
                )
                for half in range(2):
                    total = sum(
                        jnp.where(hits[j], load(s, j, half), 0.0) for j in range(FAN1)
                    )
                    at = r * width + half * LANES
                    min0[pl.ds(s, tile), at : at + LANES] = (total * share).astype(BF16)
            return 0

        lax.fori_loop(0, n_seed // tile, some, 0)

    four_means(lambda s, j, half: x1[pl.ds(8 * s + 2 * j + half, tile, stride=8), :])
    seed_part = jnp.dot(min0[...], wf[width:, :], preferred_element_type=F32)
    four_means(
        lambda s, j, half: (h1l, h1r)[half][pl.ds(FAN1 * s + j, tile, stride=FAN1), :]
    )
    second_part = jnp.dot(min0[...], ws[width:, :], preferred_element_type=F32)

    arrived(0, recv0, cap0)
    unpack(slot0_s, recv0, x0, n_seed)
    own = jnp.concatenate(
        [x0[pl.ds(0, n_seed, stride=2), :], x0[pl.ds(1, n_seed, stride=2), :]], axis=1
    ).astype(BF16)
    h1s = jnp.maximum(
        jnp.dot(own, wf[:width, :], preferred_element_type=F32) + seed_part, 0.0
    ).astype(BF16)
    second = jnp.dot(h1s, ws[:width, :], preferred_element_type=F32) + second_part

    edges = mask_ref.shape[1]
    sources = second[:edges]
    products = sources * second[edges : 2 * edges]
    positive = lax.dot_general(
        jnp.ones((8, width), F32), products, NT,
        precision=lax.Precision.HIGHEST, preferred_element_type=F32,
    )[:1]
    negative = lax.dot_general(
        second[2 * edges :], sources, NT,
        precision=lax.Precision.HIGHEST, preferred_element_type=F32,
    )
    top = jnp.maximum(jnp.max(negative, axis=0, keepdims=True), positive)
    spread = jnp.sum(jnp.exp(negative - top), axis=0, keepdims=True) + jnp.exp(positive - top)
    edge_loss = top + jnp.log(spread) - positive
    loss_ref[...] = edge_loss
    weights = mask_ref[...].astype(F32)
    left = lax.broadcasted_iota(jnp.int32, weights.shape, 1) < LANES // 2
    masked = weights * edge_loss
    both = jnp.where(
        left, masked + pltpu.roll(masked, LANES // 2, 1), weights + pltpu.roll(weights, LANES // 2, 1)
    )
    part_out[...] = both
    part_in[me] = both
    sent = req_out.at[rest]
    pltpu.make_async_copy(sent, sent, qsend).wait()
    for out, _, cap, _, h in hops:
        sent = out.at[pl.ds(0, (n - 1) * cap)]
        pltpu.make_async_copy(sent, sent, ssem.at[h]).wait()
    for t in peers:
        pltpu.make_async_remote_copy(
            src_ref=part_out, dst_ref=part_in.at[me], send_sem=psend, recv_sem=precv,
            device_id=t, device_id_type=LOGICAL,
        ).start()
    told = part_in.at[rest]
    pltpu.make_async_copy(told, told, precv).wait()
    total = jnp.sum(part_in[...], axis=0)
    loss_sum = jnp.sum(jnp.where(left, total, 0.0), axis=1, keepdims=True)
    tally = jnp.sum(jnp.where(left, 0.0, total), axis=1, keepdims=True)
    mean_ref[...] = jnp.broadcast_to(loss_sum / jnp.maximum(tally, 1.0), mean_ref.shape)
    pltpu.make_async_copy(told, told, psend).wait()


def solution(mesh):
    n = mesh.shape["dom"]

    def shards(
        features, w_first, w_second, seed_owner, seed_row, hop1_owner, hop1_row, hop1_rel,
        hop2_owner, hop2_row, hop2_rel, edge_mask,
    ):
        nodes, width = features.shape
        n_seed, n_one, n_two = seed_row.shape[0], hop1_row.shape[0], hop2_row.shape[0]
        edges = edge_mask.shape[0]
        caps = tuple(-(-2 * m // n) for m in (n_seed, n_one, n_two))
        cap0, cap1, cap2 = caps
        padded = -(-n_seed // LANES) * LANES
        vmem, hbm = pl.BlockSpec(memory_space=pltpu.VMEM), pl.BlockSpec(memory_space=pl.ANY)
        dma = pltpu.SemaphoreType.DMA

        def rows_of(cap):
            return pltpu.VMEM((n * cap, 2, LANES), BF16)

        def line(m):
            return pltpu.VMEM((1, m), jnp.int32)

        scratch = [
            line(n_seed), line(n_seed), line(n_one), line(n_one), line(n_one),
            line(n_two), line(n_two), line(n_two), line(edges),
            pltpu.VMEM((nodes, width), BF16),
            pltpu.VMEM((2 * nodes + 8, LANES), F32),
            pltpu.VMEM(w_first.shape, BF16),
            pltpu.VMEM(w_second.shape, BF16),
            pltpu.VMEM((1, padded), jnp.int32),
            pltpu.VMEM((1, padded), jnp.int32),
            pltpu.VMEM((1, padded), jnp.int32),
            pltpu.VMEM((1, n_one), jnp.int32),
            pltpu.VMEM((1, n_two), jnp.int32),
            pltpu.VMEM((n, 1, LANES), jnp.int32),
            pltpu.VMEM((n, 1, LANES), jnp.int32),
            rows_of(cap0), rows_of(cap1), rows_of(cap2),
            rows_of(cap0), rows_of(cap1), rows_of(cap2),
            pltpu.VMEM((2 * n_seed, LANES), F32),
            pltpu.VMEM((2 * n_one, LANES), F32),
            pltpu.VMEM((2 * n_two, LANES), F32),
            pltpu.VMEM((n_one, R * width), BF16),
            pltpu.VMEM((n_seed, R * width), BF16),
            pltpu.VMEM((n_one, LANES), F32),
            pltpu.VMEM((n_one, LANES), F32),
            pltpu.VMEM((n_one, LANES), F32),
            pltpu.VMEM((n_two, LANES), F32),
            pltpu.VMEM((1, edges), F32),
            pltpu.VMEM((n, 1, edges), F32),
            pltpu.SMEM((n, 1, LANES), jnp.int32),
            pltpu.SMEM((1, padded), jnp.int32),
            pltpu.SMEM((1, n_one), jnp.int32),
            pltpu.SMEM((1, n_two), jnp.int32),
            dma((9,)), dma((4,)), dma((2,)), dma, dma, dma((3,)), dma((3,)), dma((4,)), dma, dma,
        ]
        edge_loss, mean = pl.pallas_call(
            functools.partial(kernel, n, (n_seed, n_one, n_two), caps),
            out_shape=(
                jax.ShapeDtypeStruct((1, edges), F32),
                jax.ShapeDtypeStruct((1, LANES), F32),
            ),
            in_specs=[hbm] * 12,
            out_specs=(vmem, vmem),
            scratch_shapes=scratch,
            compiler_params=pltpu.CompilerParams(
                collective_id=0, has_side_effects=True, vmem_limit_bytes=62 * 2**20
            ),
            name="fetch_and_score",
        )(
            features, w_first, w_second,
            seed_owner.reshape(1, n_seed), seed_row,
            hop1_owner.reshape(1, n_one), hop1_row, hop1_rel,
            hop2_owner.reshape(1, n_two), hop2_row, hop2_rel, edge_mask,
        )
        return edge_loss.reshape(edges), mean[0, 0]

    dom = P("dom")
    tall = P("dom", None)
    return jax.shard_map(
        shards,
        mesh=mesh,
        in_specs=(tall, P(), P(), tall, dom, tall, dom, dom, tall, dom, dom, dom),
        out_specs=(dom, P()),
        check_vma=False,
    )
```

```python
import functools
import itertools

import jax
import jax.numpy as jnp
from jax import lax
from jax.experimental import pallas as pl
from jax.experimental.pallas import tpu as pltpu
from jax.sharding import PartitionSpec as P

R = 4
FAN1 = 4
FAN2 = 2
LANES = 128
SIDE = 4
NEAR = 2
LOGICAL = pl.DeviceIdType.LOGICAL
F32 = jnp.float32
BF16 = jnp.bfloat16
NT = (((1,), (1,)), ((), ()))


def kernel(
    n, count, caps,
    feat_hbm, wf_hbm, ws_hbm,
    own0_hbm, row0_hbm, own1_hbm, row1_hbm, rel1_hbm, own2_hbm, row2_hbm, rel2_hbm, mask_hbm,
    loss_ref, mean_ref,
    own0, row0, own1, row1, rel1, own2, row2, rel2, mask_ref,
    fbf, fsp, wf, ws, pad_own, pad_row, slots0, slots1, slots2, req_out, req_in,
    send0, send1, send2, recv0, recv1, recv2, x0, x1, x2, min1, min0, pre1, h1l, h1r, relc1, relc2,
    part_out, part_in,
    req_s, asker_s, slot0_s, slot1_s, slot2_s,
    isem, fsem, wsem, qsend, qrecv, ssem, rsem, tsem, psend, precv,
):
    n_seed, n_one, n_two = count
    cap0, cap1, cap2 = caps
    bases = (0, cap0, cap0 + cap1)
    me = lax.axis_index("dom")
    width = wf.shape[1]
    nodes = fbf.shape[0]
    gap = fsp.shape[0] - nodes

    lengths = (SIDE, SIDE, SIDE, 2)
    spots = []
    scale = n
    for length in lengths:
        scale //= length
        at = lax.rem(lax.div(me, scale), length)
        spots.append([lax.rem(at + d, length) * scale for d in range(length)])

    def hops_of(o):
        return sum(min(d, SIDE - d) for d in o[:3])

    offsets = sorted(
        itertools.product(*(range(length) for length in lengths)), key=lambda o: (hops_of(o) > NEAR, any(o), (((o[0] * 4 + o[1]) * 4 + o[2]) * 2 + o[3]) * 109 % 128)
    )
    close = sum(hops_of(o) <= NEAR for o in offsets)

    def at_offset(o):
        return sum(spot[d] for spot, d in zip(spots, o))

    peers = [at_offset(o) for o in offsets]
    askers = [at_offset([-d % m for d, m in zip(o, lengths)]) for o in offsets]

    here_refs = (own2, row2, own1, row1, own0, row0, rel2, rel1, mask_ref)
    there_refs = (
        own2_hbm, row2_hbm, own1_hbm, row1_hbm, own0_hbm, row0_hbm, rel2_hbm, rel1_hbm, mask_hbm
    )
    index_copies = [
        pltpu.make_async_copy(a, b if len(a.shape) == 2 else b.at[0], isem.at[i])
        for i, (a, b) in enumerate(zip(there_refs, here_refs))
    ]
    for copy in index_copies:
        copy.start()

    barrier = pltpu.get_barrier_semaphore()

    for t in peers[:0:-1]:
        pl.semaphore_signal(barrier, 1, device_id=t, device_id_type=LOGICAL)
    for k in range(n):
        asker_s[0, k] = askers[k]
    chunks = fsem.shape[0]
    part = nodes // chunks
    feat_copies = [
        pltpu.make_async_copy(
            feat_hbm.at[pl.ds(i * part, part)], fbf.at[pl.ds(i * part, part)], fsem.at[i]
        )
        for i in range(chunks)
    ]
    for copy in feat_copies:
        copy.start()
    w_copies = [
        pltpu.make_async_copy(wf_hbm, wf, wsem.at[0]),
        pltpu.make_async_copy(ws_hbm, ws, wsem.at[1]),
    ]
    for copy in w_copies:
        copy.start()

    iota_own = lax.broadcasted_iota(jnp.int32, (n, LANES), 0)
    iota_slot = lax.broadcasted_iota(jnp.int32, (64, LANES), 0)
    upper = lax.broadcasted_iota(jnp.int32, (LANES, LANES), 0) < lax.broadcasted_iota(
        jnp.int32, (LANES, LANES), 1
    )
    ladder = jnp.concatenate(
        [jnp.where(upper, 1.0, 0.0).astype(BF16), jnp.ones((LANES, LANES), BF16)], axis=1
    )

    def bucket(owner_ref, row_ref, slots, cap, base, blocks, table):
        def block(b, carry):
            before, table = carry
            cols = pl.ds(pl.multiple_of(b * LANES, LANES), LANES)
            owner = owner_ref[:, cols]
            rows = row_ref[:, cols]
            hot = jnp.where(iota_own == owner, 1.0, 0.0)
            hot16 = hot.astype(BF16)
            counts = jnp.dot(hot16, ladder, preferred_element_type=F32)
            prior = counts[:, :LANES] + before
            place = jnp.sum(hot * prior, axis=0, keepdims=True).astype(jnp.int32)
            place = jnp.clip(place, 0, cap - 1)
            slots[:, cols] = owner * cap + place
            here = iota_slot == place + base
            high = (rows >> 7).astype(F32)
            low = (rows & 127).astype(F32)
            values = jnp.concatenate(
                [jnp.where(here, high, 0.0), jnp.where(here, low, 0.0)], axis=0
            ).astype(BF16)
            table = table + lax.dot_general(hot16, values, NT, preferred_element_type=F32)
            return before + counts[:, LANES:], table

        zero = jnp.zeros((n, LANES), F32)
        return lax.fori_loop(0, blocks, block, (zero, table), unroll=9 if blocks % 9 == 0 else 3)[1]

    for copy in index_copies[:6]:
        copy.wait()
    pad_own[...] = jnp.full(pad_own.shape, -1, jnp.int32)
    pad_row[...] = jnp.zeros(pad_row.shape, jnp.int32)
    pad_own[:, :n_seed] = own0[...]
    pad_row[:, :n_seed] = row0[...]
    table = jnp.zeros((n, LANES), F32)
    table = bucket(own2, row2, slots2, cap2, bases[2], n_two // LANES, table)
    table = bucket(own1, row1, slots1, cap1, bases[1], n_one // LANES, table)
    table = bucket(pad_own, pad_row, slots0, cap0, bases[0], pad_own.shape[1] // LANES, table)
    wanted = (table * 128.0 + pltpu.roll(table, 64, 1)).astype(jnp.int32)
    wanted = jnp.clip(wanted, 0, nodes - 1)
    for i in range(n):
        req_out[i] = wanted[i : i + 1]

    def widen(i, _):
        step = 128
        r = pl.multiple_of(i * step, step)
        rows = fbf[pl.ds(r, step), :].astype(F32)
        fsp[pl.ds(r, step), :] = rows[:, :LANES]
        fsp[pl.ds(pl.multiple_of(r + gap, 8), step), :] = rows[:, LANES:]
        return 0

    per_chunk = part // 128
    feat_copies[0].wait()
    lax.fori_loop(0, per_chunk, widen, 0)

    pl.semaphore_wait(barrier, n - 1)

    for k in range(n - 1, 0, -1):
        t = peers[k]
        pltpu.make_async_remote_copy(
            src_ref=req_out.at[t], dst_ref=req_in.at[k], send_sem=qsend,
            recv_sem=qrecv.at[0 if k < close else 1], device_id=t, device_id_type=LOGICAL,
        ).start()
    req_in[0] = req_out[me]

    for i in range(1, chunks):
        feat_copies[i].wait()
        lax.fori_loop(i * per_chunk, (i + 1) * per_chunk, widen, 0)

    def asked(first, last, i):
        got = req_in.at[pl.ds(max(first, 1), last - max(first, 1))]
        pltpu.make_async_copy(got, got, qrecv.at[i]).wait()
        group = pl.ds(first, last - first)
        copy = pltpu.make_async_copy(req_in.at[group], req_s.at[group], tsem.at[i])
        copy.start()
        copy.wait()

    rest = pl.ds(0, n - 1)
    slot_copies = [
        pltpu.make_async_copy(slots2, slot2_s, tsem.at[2]),
        pltpu.make_async_copy(slots1, slot1_s, tsem.at[3]),
        pltpu.make_async_copy(slots0, slot0_s, tsem.at[4]),
    ]
    asked(0, close, 0)

    hops = ((send2, recv2, cap2, bases[2], 2), (send1, recv1, cap1, bases[1], 1), (send0, recv0, cap0, bases[0], 0))

    def gather(k, out, at, cap, base):
        for j in range(cap):
            node = req_s[k, 0, base + j]
            pair = fsp[pl.ds(node, 2, stride=gap), :]
            out[at * cap + j] = pair.astype(BF16)

    def start_send(k, out, into, cap, h):
        t = asker_s[0, k]
        pltpu.make_async_remote_copy(
            src_ref=out.at[pl.ds(k * cap, cap)], dst_ref=into.at[pl.ds(me * cap, cap)],
            send_sem=ssem.at[h], recv_sem=rsem.at[h], device_id=t, device_id_type=LOGICAL,
        ).start()

    def serve(first, last, out, into, cap, base, h):
        def one(k, _):
            gather(k, out, k, cap, base)
            start_send(k - 1, out, into, cap, h)
            return 0

        gather(first, out, first, cap, base)
        lax.fori_loop(first + 1, last, one, 0)
        start_send(last - 1, out, into, cap, h)

    out, into, cap, base, h = hops[0]
    serve(1, close, *hops[0])
    asked(close, n, 1)
    for copy in slot_copies:
        copy.start()
    serve(close, n, *hops[0])
    gather(0, into, me, cap, base)
    for out, into, cap, base, h in hops[1:]:
        serve(1, n, out, into, cap, base, h)
        gather(0, into, me, cap, base)

    for copy in index_copies[6:]:
        copy.wait()

    def relation_columns(rel_ref, out, blocks):
        def block(b, _):
            at = pl.multiple_of(b * LANES, LANES)
            row = rel_ref[:, pl.ds(at, LANES)].astype(F32)
            out[pl.ds(at, LANES), :] = jnp.broadcast_to(row, (LANES, LANES)).T
            return 0

        lax.fori_loop(0, blocks, block, 0)

    relation_columns(rel2, relc2, n_two // LANES)
    relation_columns(rel1, relc1, n_one // LANES)
    for copy in slot_copies:
        copy.wait()
    for copy in w_copies:
        copy.wait()

    def unpack(slot_s, came, out, total):
        batch = 32

        def some(b, _):
            for j in range(batch):
                i = b * batch + j
                pair = came[slot_s[0, i]].astype(F32)
                out[pl.ds(pl.multiple_of(i * 2, 2), 2), :] = pair
            return 0

        lax.fori_loop(0, total // batch, some, 0)

    def arrived(h, came, cap):
        got = came.at[pl.ds(0, (n - 1) * cap)]
        pltpu.make_async_copy(got, got, rsem.at[h]).wait()

    arrived(2, recv2, cap2)
    unpack(slot2_s, recv2, x2, n_two)
    tile = 32

    def two_means(b, _):
        f = pl.multiple_of(b * tile, tile)
        ra = relc2[pl.ds(FAN2 * f, tile, stride=FAN2), :]
        rb = relc2[pl.ds(FAN2 * f + 1, tile, stride=FAN2), :]
        share = jnp.where(ra == rb, 0.5, 1.0)
        for half in range(2):
            a = x2[pl.ds(4 * f + half, tile, stride=4), :] * share
            v = x2[pl.ds(4 * f + 2 + half, tile, stride=4), :] * share
            for r in range(R):
                mean = jnp.where(ra == r, a, 0.0) + jnp.where(rb == r, v, 0.0)
                at = r * width + half * LANES
                min1[pl.ds(f, tile), at : at + LANES] = mean.astype(BF16)
        return 0

    lax.fori_loop(0, n_one // tile, two_means, 0)

    def mean_part(b, _):
        f = pl.multiple_of(b * rows, rows)
        pre1[pl.ds(f, rows), :] = jnp.dot(
            min1[pl.ds(f, rows), :], wf[width:, :], preferred_element_type=F32
        )
        return 0

    rows = 128
    lax.fori_loop(0, n_one // rows, mean_part, 0, unroll=3)

    arrived(1, recv1, cap1)
    unpack(slot1_s, recv1, x1, n_one)

    def first_layer(b, _):
        f = pl.multiple_of(b * rows, rows)
        own = jnp.concatenate(
            [x1[pl.ds(2 * f, rows, stride=2), :], x1[pl.ds(2 * f + 1, rows, stride=2), :]], axis=1
        ).astype(BF16)
        total = jnp.dot(own, wf[:width, :], preferred_element_type=F32)
        total = total + pre1[pl.ds(f, rows), :]
        out = jnp.maximum(total, 0.0).astype(BF16).astype(F32)
        h1l[pl.ds(f, rows), :] = out[:, :LANES]
        h1r[pl.ds(f, rows), :] = out[:, LANES:]
        return 0

    lax.fori_loop(0, n_one // rows, first_layer, 0, unroll=3)

    def four_means(load):
        def some(b, _):
            s = pl.multiple_of(b * tile, tile)
            rels = [relc1[pl.ds(FAN1 * s + j, tile, stride=FAN1), :] for j in range(FAN1)]
            for r in range(R):
                hits = [rel == r for rel in rels]
                tally = sum(jnp.where(hit, 1.0, 0.0) for hit in hits)
                share = jnp.where(
                    tally == 4.0, 0.25, jnp.where(tally == 3.0, 1.0 / 3.0, jnp.where(tally == 2.0, 0.5, 1.0))
                )
                for half in range(2):
                    total = sum(
                        jnp.where(hits[j], load(s, j, half), 0.0) for j in range(FAN1)
                    )
                    at = r * width + half * LANES
                    min0[pl.ds(s, tile), at : at + LANES] = (total * share).astype(BF16)
            return 0

        lax.fori_loop(0, n_seed // tile, some, 0, unroll=3)

    four_means(lambda s, j, half: x1[pl.ds(8 * s + 2 * j + half, tile, stride=8), :])
    seed_part = jnp.dot(min0[...], wf[width:, :], preferred_element_type=F32)
    four_means(
        lambda s, j, half: (h1l, h1r)[half][pl.ds(FAN1 * s + j, tile, stride=FAN1), :]
    )
    second_part = jnp.dot(min0[...], ws[width:, :], preferred_element_type=F32)

    arrived(0, recv0, cap0)
    unpack(slot0_s, recv0, x0, n_seed)
    own = jnp.concatenate(
        [x0[pl.ds(0, n_seed, stride=2), :], x0[pl.ds(1, n_seed, stride=2), :]], axis=1
    ).astype(BF16)
    h1s = jnp.maximum(
        jnp.dot(own, wf[:width, :], preferred_element_type=F32) + seed_part, 0.0
    ).astype(BF16)
    second = jnp.dot(h1s, ws[:width, :], preferred_element_type=F32) + second_part

    edges = mask_ref.shape[1]
    sources = second[:edges]
    products = sources * second[edges : 2 * edges]
    positive = lax.dot_general(
        jnp.ones((8, width), F32), products, NT,
        precision=lax.Precision.HIGHEST, preferred_element_type=F32,
    )[:1]
    negative = lax.dot_general(
        second[2 * edges :], sources, NT,
        precision=lax.Precision.HIGHEST, preferred_element_type=F32,
    )
    top = jnp.maximum(jnp.max(negative, axis=0, keepdims=True), positive)
    spread = jnp.sum(jnp.exp(negative - top), axis=0, keepdims=True) + jnp.exp(positive - top)
    edge_loss = top + jnp.log(spread) - positive
    loss_ref[...] = edge_loss
    weights = mask_ref[...].astype(F32)
    left = lax.broadcasted_iota(jnp.int32, weights.shape, 1) < LANES // 2
    masked = weights * edge_loss
    both = jnp.where(
        left, masked + pltpu.roll(masked, LANES // 2, 1), weights + pltpu.roll(weights, LANES // 2, 1)
    )
    part_out[...] = both
    part_in[me] = both
    for t in peers[:0:-1]:
        pltpu.make_async_remote_copy(
            src_ref=part_out, dst_ref=part_in.at[me], send_sem=psend, recv_sem=precv,
            device_id=t, device_id_type=LOGICAL,
        ).start()
    told = part_in.at[rest]
    pltpu.make_async_copy(told, told, precv).wait()
    total = jnp.sum(part_in[...], axis=0)
    loss_sum = jnp.sum(jnp.where(left, total, 0.0), axis=1, keepdims=True)
    tally = jnp.sum(jnp.where(left, 0.0, total), axis=1, keepdims=True)
    mean_ref[...] = jnp.broadcast_to(loss_sum / jnp.maximum(tally, 1.0), mean_ref.shape)
    pltpu.make_async_copy(told, told, psend).wait()
    sent = req_out.at[rest]
    pltpu.make_async_copy(sent, sent, qsend).wait()
    for out, _, cap, _, h in hops:
        sent = out.at[pl.ds(0, (n - 1) * cap)]
        pltpu.make_async_copy(sent, sent, ssem.at[h]).wait()


def solution(mesh):
    n = mesh.shape["dom"]

    def shards(
        features, w_first, w_second, seed_owner, seed_row, hop1_owner, hop1_row, hop1_rel,
        hop2_owner, hop2_row, hop2_rel, edge_mask,
    ):
        nodes, width = features.shape
        n_seed, n_one, n_two = seed_row.shape[0], hop1_row.shape[0], hop2_row.shape[0]
        edges = edge_mask.shape[0]
        caps = tuple(-(-2 * m // n) for m in (n_seed, n_one, n_two))
        cap0, cap1, cap2 = caps
        padded = -(-n_seed // LANES) * LANES
        vmem, hbm = pl.BlockSpec(memory_space=pltpu.VMEM), pl.BlockSpec(memory_space=pl.ANY)
        dma = pltpu.SemaphoreType.DMA

        def rows_of(cap):
            return pltpu.VMEM((n * cap, 2, LANES), BF16)

        def line(m):
            return pltpu.VMEM((1, m), jnp.int32)

        scratch = [
            line(n_seed), line(n_seed), line(n_one), line(n_one), line(n_one),
            line(n_two), line(n_two), line(n_two), line(edges),
            pltpu.VMEM((nodes, width), BF16),
            pltpu.VMEM((2 * nodes + 8, LANES), F32),
            pltpu.VMEM(w_first.shape, BF16),
            pltpu.VMEM(w_second.shape, BF16),
            pltpu.VMEM((1, padded), jnp.int32),
            pltpu.VMEM((1, padded), jnp.int32),
            pltpu.VMEM((1, padded), jnp.int32),
            pltpu.VMEM((1, n_one), jnp.int32),
            pltpu.VMEM((1, n_two), jnp.int32),
            pltpu.VMEM((n, 1, LANES), jnp.int32),
            pltpu.VMEM((n, 1, LANES), jnp.int32),
            rows_of(cap0), rows_of(cap1), rows_of(cap2),
            rows_of(cap0), rows_of(cap1), rows_of(cap2),
            pltpu.VMEM((2 * n_seed, LANES), F32),
            pltpu.VMEM((2 * n_one, LANES), F32),
            pltpu.VMEM((2 * n_two, LANES), F32),
            pltpu.VMEM((n_one, R * width), BF16),
            pltpu.VMEM((n_seed, R * width), BF16),
            pltpu.VMEM((n_one, width), F32),
            pltpu.VMEM((n_one, LANES), F32),
            pltpu.VMEM((n_one, LANES), F32),
            pltpu.VMEM((n_one, LANES), F32),
            pltpu.VMEM((n_two, LANES), F32),
            pltpu.VMEM((1, edges), F32),
            pltpu.VMEM((n, 1, edges), F32),
            pltpu.SMEM((n, 1, LANES), jnp.int32),
            pltpu.SMEM((1, n), jnp.int32),
            pltpu.SMEM((1, padded), jnp.int32),
            pltpu.SMEM((1, n_one), jnp.int32),
            pltpu.SMEM((1, n_two), jnp.int32),
            dma((9,)), dma((4,)), dma((2,)), dma, dma((2,)), dma((3,)), dma((3,)), dma((5,)), dma, dma,
        ]
        edge_loss, mean = pl.pallas_call(
            functools.partial(kernel, n, (n_seed, n_one, n_two), caps),
            out_shape=(
                jax.ShapeDtypeStruct((1, edges), F32),
                jax.ShapeDtypeStruct((1, LANES), F32),
            ),
            in_specs=[hbm] * 12,
            out_specs=(vmem, vmem),
            scratch_shapes=scratch,
            compiler_params=pltpu.CompilerParams(
                collective_id=0, has_side_effects=True, vmem_limit_bytes=62 * 2**20
            ),
            name="fetch_and_score",
        )(
            features, w_first, w_second,
            seed_owner.reshape(1, n_seed), seed_row,
            hop1_owner.reshape(1, n_one), hop1_row, hop1_rel,
            hop2_owner.reshape(1, n_two), hop2_row, hop2_rel, edge_mask,
        )
        return edge_loss.reshape(edges), mean[0, 0]

    dom = P("dom")
    tall = P("dom", None)
    return jax.shard_map(
        shards,
        mesh=mesh,
        in_specs=(tall, P(), P(), tall, dom, tall, dom, dom, tall, dom, dom, dom),
        out_specs=(dom, P()),
        check_vma=False,
    )
```

```python
import functools
import itertools

import jax
import jax.numpy as jnp
from jax import lax
from jax.experimental import pallas as pl
from jax.experimental.pallas import tpu as pltpu
from jax.sharding import PartitionSpec as P

R = 4
FAN1 = 4
FAN2 = 2
LANES = 128
SIDE = 4
NEAR = 2
LOGICAL = pl.DeviceIdType.LOGICAL
F32 = jnp.float32
BF16 = jnp.bfloat16
NT = (((1,), (1,)), ((), ()))


def kernel(
    n, count, caps,
    feat_hbm, wf_hbm, ws_hbm,
    own0_hbm, row0_hbm, own1_hbm, row1_hbm, rel1_hbm, own2_hbm, row2_hbm, rel2_hbm, mask_hbm,
    loss_ref, mean_ref,
    own0, row0, own1, row1, rel1, own2, row2, rel2, mask_ref,
    fbf, fsp, wf, ws, pad_own, pad_row, slots0, slots1, slots2, req_out, req_in,
    send0, send1, send2, recv0, recv1, recv2, x0, x1, x2, min1, min0x, min0h, pre1, pick1, share1, relc2,
    part_out, part_in,
    req_s, asker_s, slot0_s, slot1_s, slot2_s,
    isem, fsem, wsem, qsend, qrecv, ssem, rsem, tsem, psend, precv,
):
    n_seed, n_one, n_two = count
    cap0, cap1, cap2 = caps
    bases = (0, cap0, cap0 + cap1)
    me = lax.axis_index("dom")
    width = wf.shape[1]
    nodes = fbf.shape[0]
    gap = fsp.shape[0] - nodes

    lengths = (SIDE, SIDE, SIDE, 2)
    spots = []
    scale = n
    for length in lengths:
        scale //= length
        at = lax.rem(lax.div(me, scale), length)
        spots.append([lax.rem(at + d, length) * scale for d in range(length)])

    def hops_of(o):
        return sum(min(d, SIDE - d) for d in o[:3])

    offsets = sorted(
        itertools.product(*(range(length) for length in lengths)), key=lambda o: (hops_of(o) > NEAR, any(o), (((o[0] * 4 + o[1]) * 4 + o[2]) * 2 + o[3]) * 109 % 128)
    )
    close = sum(hops_of(o) <= NEAR for o in offsets)

    def at_offset(o):
        return sum(spot[d] for spot, d in zip(spots, o))

    peers = [at_offset(o) for o in offsets]
    askers = [at_offset([-d % m for d, m in zip(o, lengths)]) for o in offsets]

    here_refs = (own2, row2, own1, row1, own0, row0, rel2, rel1, mask_ref)
    there_refs = (
        own2_hbm, row2_hbm, own1_hbm, row1_hbm, own0_hbm, row0_hbm, rel2_hbm, rel1_hbm, mask_hbm
    )
    index_copies = [
        pltpu.make_async_copy(a, b if len(a.shape) == 2 else b.at[0], isem.at[i])
        for i, (a, b) in enumerate(zip(there_refs, here_refs))
    ]
    for copy in index_copies:
        copy.start()

    barrier = pltpu.get_barrier_semaphore()

    for t in peers[:0:-1]:
        pl.semaphore_signal(barrier, 1, device_id=t, device_id_type=LOGICAL)
    for k in range(n):
        asker_s[0, k] = askers[k]
    chunks = fsem.shape[0]
    part = nodes // chunks
    feat_copies = [
        pltpu.make_async_copy(
            feat_hbm.at[pl.ds(i * part, part)], fbf.at[pl.ds(i * part, part)], fsem.at[i]
        )
        for i in range(chunks)
    ]
    for copy in feat_copies:
        copy.start()
    w_copies = [
        pltpu.make_async_copy(wf_hbm, wf, wsem.at[0]),
        pltpu.make_async_copy(ws_hbm, ws, wsem.at[1]),
    ]
    for copy in w_copies:
        copy.start()

    iota_own = lax.broadcasted_iota(jnp.int32, (n, LANES), 0)
    iota_slot = lax.broadcasted_iota(jnp.int32, (64, LANES), 0)
    upper = lax.broadcasted_iota(jnp.int32, (LANES, LANES), 0) < lax.broadcasted_iota(
        jnp.int32, (LANES, LANES), 1
    )
    ladder = jnp.concatenate(
        [jnp.where(upper, 1.0, 0.0).astype(BF16), jnp.ones((LANES, LANES), BF16)], axis=1
    )

    def bucket(owner_ref, row_ref, slots, cap, base, blocks, table):
        def block(b, carry):
            before, table = carry
            cols = pl.ds(pl.multiple_of(b * LANES, LANES), LANES)
            owner = owner_ref[:, cols]
            rows = row_ref[:, cols]
            hot = jnp.where(iota_own == owner, 1.0, 0.0)
            hot16 = hot.astype(BF16)
            counts = jnp.dot(hot16, ladder, preferred_element_type=F32)
            prior = counts[:, :LANES] + before
            place = jnp.sum(hot * prior, axis=0, keepdims=True).astype(jnp.int32)
            place = jnp.clip(place, 0, cap - 1)
            slots[:, cols] = owner * cap + place
            here = iota_slot == place + base
            high = (rows >> 7).astype(F32)
            low = (rows & 127).astype(F32)
            values = jnp.concatenate(
                [jnp.where(here, high, 0.0), jnp.where(here, low, 0.0)], axis=0
            ).astype(BF16)
            table = table + lax.dot_general(hot16, values, NT, preferred_element_type=F32)
            return before + counts[:, LANES:], table

        zero = jnp.zeros((n, LANES), F32)
        return lax.fori_loop(0, blocks, block, (zero, table), unroll=9 if blocks % 9 == 0 else 3)[1]

    for copy in index_copies[:6]:
        copy.wait()
    pad_own[...] = jnp.full(pad_own.shape, -1, jnp.int32)
    pad_row[...] = jnp.zeros(pad_row.shape, jnp.int32)
    pad_own[:, :n_seed] = own0[...]
    pad_row[:, :n_seed] = row0[...]
    table = jnp.zeros((n, LANES), F32)
    table = bucket(own2, row2, slots2, cap2, bases[2], n_two // LANES, table)
    table = bucket(own1, row1, slots1, cap1, bases[1], n_one // LANES, table)
    table = bucket(pad_own, pad_row, slots0, cap0, bases[0], pad_own.shape[1] // LANES, table)
    wanted = (table * 128.0 + pltpu.roll(table, 64, 1)).astype(jnp.int32)
    wanted = jnp.clip(wanted, 0, nodes - 1)
    for i in range(n):
        req_out[i] = wanted[i : i + 1]

    def widen(i, _):
        step = 128
        r = pl.multiple_of(i * step, step)
        rows = fbf[pl.ds(r, step), :].astype(F32)
        fsp[pl.ds(r, step), :] = rows[:, :LANES]
        fsp[pl.ds(pl.multiple_of(r + gap, 8), step), :] = rows[:, LANES:]
        return 0

    per_chunk = part // 128
    feat_copies[0].wait()
    lax.fori_loop(0, per_chunk, widen, 0)

    pl.semaphore_wait(barrier, n - 1)

    for k in range(1, n):
        t = peers[k]
        pltpu.make_async_remote_copy(
            src_ref=req_out.at[t], dst_ref=req_in.at[k], send_sem=qsend,
            recv_sem=qrecv.at[0 if k < close else 1], device_id=t, device_id_type=LOGICAL,
        ).start()
    req_in[0] = req_out[me]

    for i in range(1, chunks):
        feat_copies[i].wait()
        lax.fori_loop(i * per_chunk, (i + 1) * per_chunk, widen, 0)

    def asked(first, last, i):
        got = req_in.at[pl.ds(max(first, 1), last - max(first, 1))]
        pltpu.make_async_copy(got, got, qrecv.at[i]).wait()
        group = pl.ds(first, last - first)
        copy = pltpu.make_async_copy(req_in.at[group], req_s.at[group], tsem.at[i])
        copy.start()
        copy.wait()

    rest = pl.ds(0, n - 1)
    slot_copies = [
        pltpu.make_async_copy(slots2, slot2_s, tsem.at[2]),
        pltpu.make_async_copy(slots1, slot1_s, tsem.at[3]),
        pltpu.make_async_copy(slots0, slot0_s, tsem.at[4]),
    ]
    asked(0, close, 0)

    hops = ((send2, recv2, cap2, bases[2], 2), (send1, recv1, cap1, bases[1], 1), (send0, recv0, cap0, bases[0], 0))

    def gather(k, out, at, cap, base):
        for j in range(cap):
            node = req_s[k, 0, base + j]
            pair = fsp[pl.ds(node, 2, stride=gap), :]
            out[at * cap + j] = pair.astype(BF16)

    def start_send(k, out, into, cap, h):
        t = asker_s[0, k]
        pltpu.make_async_remote_copy(
            src_ref=out.at[pl.ds(k * cap, cap)], dst_ref=into.at[pl.ds(me * cap, cap)],
            send_sem=ssem.at[h], recv_sem=rsem.at[h], device_id=t, device_id_type=LOGICAL,
        ).start()

    def serve(first, last, out, into, cap, base, h):
        def one(k, _):
            gather(k, out, k, cap, base)
            start_send(k - 1, out, into, cap, h)
            return 0

        gather(first, out, first, cap, base)
        lax.fori_loop(first + 1, last, one, 0)
        start_send(last - 1, out, into, cap, h)

    def serve_back(first, last, out, into, cap, base, h):
        def one(i, _):
            k = last - 1 - i
            gather(k, out, k, cap, base)
            start_send(k + 1, out, into, cap, h)
            return 0

        gather(last - 1, out, last - 1, cap, base)
        lax.fori_loop(1, last - first, one, 0)
        start_send(first, out, into, cap, h)

    out, into, cap, base, h = hops[0]
    serve(1, close, *hops[0])
    asked(close, n, 1)
    for copy in slot_copies:
        copy.start()
    serve(close, n, *hops[0])
    gather(0, into, me, cap, base)
    for out, into, cap, base, h in hops[1:]:
        serve(1, n, out, into, cap, base, h)
        gather(0, into, me, cap, base)

    for copy in index_copies[6:]:
        copy.wait()

    def relation_columns(rel_ref, out, blocks):
        def block(b, _):
            at = pl.multiple_of(b * LANES, LANES)
            row = rel_ref[:, pl.ds(at, LANES)].astype(F32)
            out[pl.ds(at, LANES), :] = jnp.broadcast_to(row, (LANES, LANES)).T
            return 0

        lax.fori_loop(0, blocks, block, 0)

    relation_columns(rel2, relc2, n_two // LANES)

    def seed_picks(b, _):
        at = pl.multiple_of(b * LANES, LANES)
        rel = rel1[:, pl.ds(at, LANES)]
        shape = (LANES // FAN1, LANES)
        first = lax.broadcasted_iota(jnp.int32, shape, 0) * FAN1
        ahead = lax.broadcasted_iota(jnp.int32, shape, 1) - first
        mine = (ahead >= 0) & (ahead < FAN1)
        pick = jnp.concatenate(
            [jnp.where(mine & (rel == r), 1.0, 0.0) for r in range(R)], axis=0
        ).astype(BF16)
        pick1[pl.ds(at, LANES), :] = pick
        tally = jnp.dot(pick, jnp.ones((LANES, LANES), BF16), preferred_element_type=F32)
        share1[pl.ds(at, LANES), :] = jnp.where(
            tally == 4.0, 0.25, jnp.where(tally == 3.0, 1.0 / 3.0, jnp.where(tally == 2.0, 0.5, 1.0))
        )
        return 0

    lax.fori_loop(0, n_one // LANES, seed_picks, 0)
    for copy in slot_copies:
        copy.wait()
    for copy in w_copies:
        copy.wait()

    def unpack(slot_s, came, out, total):
        batch = 32

        def some(b, _):
            for j in range(batch):
                i = b * batch + j
                pair = came[slot_s[0, i]].astype(F32)
                out[pl.ds(pl.multiple_of(i * 2, 2), 2), :] = pair
            return 0

        lax.fori_loop(0, total // batch, some, 0)

    def arrived(h, came, cap):
        got = came.at[pl.ds(0, (n - 1) * cap)]
        pltpu.make_async_copy(got, got, rsem.at[h]).wait()

    arrived(2, recv2, cap2)
    unpack(slot2_s, recv2, x2, n_two)
    tile = 32

    def two_means(b, _):
        f = pl.multiple_of(b * tile, tile)
        ra = relc2[pl.ds(FAN2 * f, tile, stride=FAN2), :]
        rb = relc2[pl.ds(FAN2 * f + 1, tile, stride=FAN2), :]
        share = jnp.where(ra == rb, 0.5, 1.0)
        for half in range(2):
            a = x2[pl.ds(4 * f + half, tile, stride=4), :] * share
            v = x2[pl.ds(4 * f + 2 + half, tile, stride=4), :] * share
            for r in range(R):
                mean = jnp.where(ra == r, a, 0.0) + jnp.where(rb == r, v, 0.0)
                at = r * width + half * LANES
                min1[pl.ds(f, tile), at : at + LANES] = mean.astype(BF16)
        return 0

    lax.fori_loop(0, n_one // tile, two_means, 0)

    def mean_part(b, _):
        f = pl.multiple_of(b * rows, rows)
        pre1[pl.ds(f, rows), :] = jnp.dot(
            min1[pl.ds(f, rows), :], wf[width:, :], preferred_element_type=F32
        )
        return 0

    rows = 128
    lax.fori_loop(0, n_one // rows, mean_part, 0, unroll=3)

    arrived(1, recv1, cap1)
    unpack(slot1_s, recv1, x1, n_one)

    def first_layer(b, _):
        f = pl.multiple_of(b * rows, rows)
        own = jnp.concatenate(
            [x1[pl.ds(2 * f, rows, stride=2), :], x1[pl.ds(2 * f + 1, rows, stride=2), :]], axis=1
        ).astype(BF16)
        total = jnp.dot(own, wf[:width, :], preferred_element_type=F32)
        total = total + pre1[pl.ds(f, rows), :]
        out = jnp.maximum(total, 0.0).astype(BF16)
        pick = pick1[pl.ds(f, rows), :]
        share = share1[pl.ds(f, rows), :]
        s = pl.multiple_of(b * tile, tile)
        for values, means in ((own, min0x), (out, min0h)):
            sums = jnp.dot(pick, values, preferred_element_type=F32)
            for r in range(R):
                for at in range(0, width, LANES):
                    mean = sums[r * tile : (r + 1) * tile, at : at + LANES] * share[r * tile : (r + 1) * tile]
                    means[pl.ds(s, tile), r * width + at : r * width + at + LANES] = mean.astype(BF16)
        return 0

    lax.fori_loop(0, n_one // rows, first_layer, 0, unroll=3)

    seed_part = jnp.dot(min0x[...], wf[width:, :], preferred_element_type=F32)
    second_part = jnp.dot(min0h[...], ws[width:, :], preferred_element_type=F32)

    arrived(0, recv0, cap0)
    unpack(slot0_s, recv0, x0, n_seed)
    own = jnp.concatenate(
        [x0[pl.ds(0, n_seed, stride=2), :], x0[pl.ds(1, n_seed, stride=2), :]], axis=1
    ).astype(BF16)
    h1s = jnp.maximum(
        jnp.dot(own, wf[:width, :], preferred_element_type=F32) + seed_part, 0.0
    ).astype(BF16)
    second = jnp.dot(h1s, ws[:width, :], preferred_element_type=F32) + second_part

    edges = mask_ref.shape[1]
    sources = second[:edges]
    products = sources * second[edges : 2 * edges]
    positive = lax.dot_general(
        jnp.ones((8, width), F32), products, NT,
        precision=lax.Precision.HIGHEST, preferred_element_type=F32,
    )[:1]
    negative = lax.dot_general(
        second[2 * edges :], sources, NT,
        precision=lax.Precision.HIGHEST, preferred_element_type=F32,
    )
    top = jnp.maximum(jnp.max(negative, axis=0, keepdims=True), positive)
    spread = jnp.sum(jnp.exp(negative - top), axis=0, keepdims=True) + jnp.exp(positive - top)
    edge_loss = top + jnp.log(spread) - positive
    loss_ref[...] = edge_loss
    weights = mask_ref[...].astype(F32)
    left = lax.broadcasted_iota(jnp.int32, weights.shape, 1) < LANES // 2
    masked = weights * edge_loss
    both = jnp.where(
        left, masked + pltpu.roll(masked, LANES // 2, 1), weights + pltpu.roll(weights, LANES // 2, 1)
    )
    part_out[...] = both
    part_in[me] = both
    for t in peers[:0:-1]:
        pltpu.make_async_remote_copy(
            src_ref=part_out, dst_ref=part_in.at[me], send_sem=psend, recv_sem=precv,
            device_id=t, device_id_type=LOGICAL,
        ).start()
    told = part_in.at[rest]
    pltpu.make_async_copy(told, told, precv).wait()
    total = jnp.sum(part_in[...], axis=0)
    loss_sum = jnp.sum(jnp.where(left, total, 0.0), axis=1, keepdims=True)
    tally = jnp.sum(jnp.where(left, 0.0, total), axis=1, keepdims=True)
    mean_ref[...] = jnp.broadcast_to(loss_sum / jnp.maximum(tally, 1.0), mean_ref.shape)
    pltpu.make_async_copy(told, told, psend).wait()
    sent = req_out.at[rest]
    pltpu.make_async_copy(sent, sent, qsend).wait()
    for out, _, cap, _, h in hops:
        sent = out.at[pl.ds(0, (n - 1) * cap)]
        pltpu.make_async_copy(sent, sent, ssem.at[h]).wait()


def solution(mesh):
    n = mesh.shape["dom"]

    def shards(
        features, w_first, w_second, seed_owner, seed_row, hop1_owner, hop1_row, hop1_rel,
        hop2_owner, hop2_row, hop2_rel, edge_mask,
    ):
        nodes, width = features.shape
        n_seed, n_one, n_two = seed_row.shape[0], hop1_row.shape[0], hop2_row.shape[0]
        edges = edge_mask.shape[0]
        caps = tuple(-(-2 * m // n) for m in (n_seed, n_one, n_two))
        cap0, cap1, cap2 = caps
        padded = -(-n_seed // LANES) * LANES
        vmem, hbm = pl.BlockSpec(memory_space=pltpu.VMEM), pl.BlockSpec(memory_space=pl.ANY)
        dma = pltpu.SemaphoreType.DMA

        def rows_of(cap):
            return pltpu.VMEM((n * cap, 2, LANES), BF16)

        def line(m):
            return pltpu.VMEM((1, m), jnp.int32)

        scratch = [
            line(n_seed), line(n_seed), line(n_one), line(n_one), line(n_one),
            line(n_two), line(n_two), line(n_two), line(edges),
            pltpu.VMEM((nodes, width), BF16),
            pltpu.VMEM((2 * nodes + 8, LANES), F32),
            pltpu.VMEM(w_first.shape, BF16),
            pltpu.VMEM(w_second.shape, BF16),
            pltpu.VMEM((1, padded), jnp.int32),
            pltpu.VMEM((1, padded), jnp.int32),
            pltpu.VMEM((1, padded), jnp.int32),
            pltpu.VMEM((1, n_one), jnp.int32),
            pltpu.VMEM((1, n_two), jnp.int32),
            pltpu.VMEM((n, 1, LANES), jnp.int32),
            pltpu.VMEM((n, 1, LANES), jnp.int32),
            rows_of(cap0), rows_of(cap1), rows_of(cap2),
            rows_of(cap0), rows_of(cap1), rows_of(cap2),
            pltpu.VMEM((2 * n_seed, LANES), F32),
            pltpu.VMEM((2 * n_one, LANES), F32),
            pltpu.VMEM((2 * n_two, LANES), F32),
            pltpu.VMEM((n_one, R * width), BF16),
            pltpu.VMEM((n_seed, R * width), BF16),
            pltpu.VMEM((n_seed, R * width), BF16),
            pltpu.VMEM((n_one, width), F32),
            pltpu.VMEM((n_one, LANES), BF16),
            pltpu.VMEM((n_one, LANES), F32),
            pltpu.VMEM((n_two, LANES), F32),
            pltpu.VMEM((1, edges), F32),
            pltpu.VMEM((n, 1, edges), F32),
            pltpu.SMEM((n, 1, LANES), jnp.int32),
            pltpu.SMEM((1, n), jnp.int32),
            pltpu.SMEM((1, padded), jnp.int32),
            pltpu.SMEM((1, n_one), jnp.int32),
            pltpu.SMEM((1, n_two), jnp.int32),
            dma((9,)), dma((4,)), dma((2,)), dma, dma((2,)), dma((3,)), dma((3,)), dma((5,)), dma, dma,
        ]
        edge_loss, mean = pl.pallas_call(
            functools.partial(kernel, n, (n_seed, n_one, n_two), caps),
            out_shape=(
                jax.ShapeDtypeStruct((1, edges), F32),
                jax.ShapeDtypeStruct((1, LANES), F32),
            ),
            in_specs=[hbm] * 12,
            out_specs=(vmem, vmem),
            scratch_shapes=scratch,
            compiler_params=pltpu.CompilerParams(
                collective_id=0, has_side_effects=True, vmem_limit_bytes=62 * 2**20
            ),
            name="fetch_and_score",
        )(
            features, w_first, w_second,
            seed_owner.reshape(1, n_seed), seed_row,
            hop1_owner.reshape(1, n_one), hop1_row, hop1_rel,
            hop2_owner.reshape(1, n_two), hop2_row, hop2_rel, edge_mask,
        )
        return edge_loss.reshape(edges), mean[0, 0]

    dom = P("dom")
    tall = P("dom", None)
    return jax.shard_map(
        shards,
        mesh=mesh,
        in_specs=(tall, P(), P(), tall, dom, tall, dom, dom, tall, dom, dom, dom),
        out_specs=(dom, P()),
        check_vma=False,
    )
```

```python
import functools
import itertools

import jax
import jax.numpy as jnp
from jax import lax
from jax.experimental import pallas as pl
from jax.experimental.pallas import tpu as pltpu
from jax.sharding import PartitionSpec as P

R = 4
FAN1 = 4
FAN2 = 2
LANES = 128
SIDE = 4
NEAR = 2
LOGICAL = pl.DeviceIdType.LOGICAL
F32 = jnp.float32
BF16 = jnp.bfloat16
NT = (((1,), (1,)), ((), ()))


def kernel(
    n, count, caps,
    feat_hbm, wf_hbm, ws_hbm,
    own0_hbm, row0_hbm, own1_hbm, row1_hbm, rel1_hbm, own2_hbm, row2_hbm, rel2_hbm, mask_hbm,
    result_ref,
    own0, row0, own1, row1, rel1, own2, row2, rel2, mask_ref,
    fbf, fsp, wf, ws, pad_own, pad_row, slots0, slots1, slots2, req_out, req_in,
    send0, send1, send2, recv0, recv1, recv2, x0, x1, x2, min1, min0x, min0h, pre1, pick1, share1, relc2,
    part_out, part_in,
    req_s, asker_s, slot0_s, slot1_s, slot2_s,
    isem, fsem, wsem, qsend, qrecv, ssem, rsem, tsem, psend, precv,
):
    n_seed, n_one, n_two = count
    cap0, cap1, cap2 = caps
    bases = (0, cap0, cap0 + cap1)
    me = lax.axis_index("dom")
    width = wf.shape[1]
    nodes = fbf.shape[0]
    gap = fsp.shape[0] - nodes

    lengths = (SIDE, SIDE, SIDE, 2)
    scales = [2 * SIDE * SIDE, 2 * SIDE, 2, 1]
    ats = [lax.rem(lax.div(me, scale), length) for scale, length in zip(scales, lengths)]
    core = ats[3]
    toward, away = [], []
    for sender in (core, 1 - core):
        toward.append([])
        away.append([])
        for at, scale in zip(ats[:3], scales):
            turn = [d + sender * (SIDE - 2 * d) for d in range(SIDE)]
            toward[-1].append([lax.rem(at + t, SIDE) * scale for t in turn])
            away[-1].append([lax.rem(at + 2 * SIDE - t, SIDE) * scale for t in turn])

    def hops_of(o):
        return sum(min(d, SIDE - d) for d in o[:3])

    offsets = sorted(
        itertools.product(*(range(length) for length in lengths)), key=lambda o: (hops_of(o) > NEAR, any(o), (((o[0] * 4 + o[1]) * 4 + o[2]) * 2 + o[3]) * 45 % 128)
    )
    close = sum(hops_of(o) <= NEAR for o in offsets)

    def other(table, o):
        return sum(spot[d] for spot, d in zip(table, o)) + (1 - core if o[3] else core)

    peers = [other(toward[0], o) for o in offsets]
    askers = [other(away[o[3]], o) for o in offsets]

    here_refs = (own2, row2, own1, row1, own0, row0, rel2, rel1, mask_ref)
    there_refs = (
        own2_hbm, row2_hbm, own1_hbm, row1_hbm, own0_hbm, row0_hbm, rel2_hbm, rel1_hbm, mask_hbm
    )
    index_copies = [
        pltpu.make_async_copy(a, b if len(a.shape) == 2 else b.at[0], isem.at[i])
        for i, (a, b) in enumerate(zip(there_refs, here_refs))
    ]
    for copy in index_copies:
        copy.start()

    chunks = fsem.shape[0]
    part = nodes // chunks
    feat_copies = [
        pltpu.make_async_copy(
            feat_hbm.at[pl.ds(i * part, part)], fbf.at[pl.ds(i * part, part)], fsem.at[i]
        )
        for i in range(chunks)
    ]
    for copy in feat_copies:
        copy.start()
    barrier = pltpu.get_barrier_semaphore()

    for t in peers[:0:-1]:
        pl.semaphore_signal(barrier, 1, device_id=t, device_id_type=LOGICAL)
    for k in range(n):
        asker_s[0, k] = askers[k]
    w_copies = [
        pltpu.make_async_copy(wf_hbm, wf, wsem.at[0]),
        pltpu.make_async_copy(ws_hbm, ws, wsem.at[1]),
    ]
    for copy in w_copies:
        copy.start()

    iota_own = lax.broadcasted_iota(jnp.int32, (n, LANES), 0)
    iota_slot = lax.broadcasted_iota(jnp.int32, (64, LANES), 0)
    upper = lax.broadcasted_iota(jnp.int32, (LANES, LANES), 0) < lax.broadcasted_iota(
        jnp.int32, (LANES, LANES), 1
    )
    ladder = jnp.concatenate(
        [jnp.where(upper, 1.0, 0.0).astype(BF16), jnp.ones((LANES, LANES), BF16)], axis=1
    )

    def bucket(owner_ref, row_ref, slots, cap, base, blocks, table):
        def block(b, carry):
            before, table = carry
            cols = pl.ds(pl.multiple_of(b * LANES, LANES), LANES)
            owner = owner_ref[:, cols]
            rows = row_ref[:, cols]
            hot = jnp.where(iota_own == owner, 1.0, 0.0)
            hot16 = hot.astype(BF16)
            counts = jnp.dot(hot16, ladder, preferred_element_type=F32)
            prior = counts[:, :LANES] + before
            place = jnp.sum(hot * prior, axis=0, keepdims=True).astype(jnp.int32)
            place = jnp.clip(place, 0, cap - 1)
            slots[:, cols] = owner * cap + place
            here = iota_slot == place + base
            high = (rows >> 7).astype(F32)
            low = (rows & 127).astype(F32)
            values = jnp.concatenate(
                [jnp.where(here, high, 0.0), jnp.where(here, low, 0.0)], axis=0
            ).astype(BF16)
            table = table + lax.dot_general(hot16, values, NT, preferred_element_type=F32)
            return before + counts[:, LANES:], table

        zero = jnp.zeros((n, LANES), F32)
        return lax.fori_loop(0, blocks, block, (zero, table), unroll=9 if blocks % 9 == 0 else 3)[1]

    for copy in index_copies[:6]:
        copy.wait()
    pad_own[...] = jnp.full(pad_own.shape, -1, jnp.int32)
    pad_row[...] = jnp.zeros(pad_row.shape, jnp.int32)
    pad_own[:, :n_seed] = own0[...]
    pad_row[:, :n_seed] = row0[...]
    table = jnp.zeros((n, LANES), F32)
    table = bucket(own2, row2, slots2, cap2, bases[2], n_two // LANES, table)
    table = bucket(own1, row1, slots1, cap1, bases[1], n_one // LANES, table)
    table = bucket(pad_own, pad_row, slots0, cap0, bases[0], pad_own.shape[1] // LANES, table)
    wanted = (table * 128.0 + pltpu.roll(table, 64, 1)).astype(jnp.int32)
    wanted = jnp.clip(wanted, 0, nodes - 1)
    for i in range(n):
        req_out[i] = wanted[i : i + 1]

    def widen(i, _):
        step = 128
        r = pl.multiple_of(i * step, step)
        rows = fbf[pl.ds(r, step), :].astype(F32)
        fsp[pl.ds(r, step), :] = rows[:, :LANES]
        fsp[pl.ds(pl.multiple_of(r + gap, 8), step), :] = rows[:, LANES:]
        return 0

    per_chunk = part // 128
    feat_copies[0].wait()
    lax.fori_loop(0, per_chunk, widen, 0)

    pl.semaphore_wait(barrier, n - 1)

    for k in range(1, n):
        t = peers[k]
        pltpu.make_async_remote_copy(
            src_ref=req_out.at[t], dst_ref=req_in.at[k], send_sem=qsend,
            recv_sem=qrecv.at[0 if k < close else 1], device_id=t, device_id_type=LOGICAL,
        ).start()
    req_in[0] = req_out[me]

    for i in range(1, chunks):
        feat_copies[i].wait()
        lax.fori_loop(i * per_chunk, (i + 1) * per_chunk, widen, 0)

    def asked(first, last, i):
        got = req_in.at[pl.ds(max(first, 1), last - max(first, 1))]
        pltpu.make_async_copy(got, got, qrecv.at[i]).wait()
        group = pl.ds(first, last - first)
        copy = pltpu.make_async_copy(req_in.at[group], req_s.at[group], tsem.at[i])
        copy.start()
        copy.wait()

    rest = pl.ds(0, n - 1)
    slot_copies = [
        pltpu.make_async_copy(slots2, slot2_s, tsem.at[2]),
        pltpu.make_async_copy(slots1, slot1_s, tsem.at[3]),
        pltpu.make_async_copy(slots0, slot0_s, tsem.at[4]),
    ]
    asked(0, close, 0)

    hops = ((send2, recv2, cap2, bases[2], 2), (send1, recv1, cap1, bases[1], 1), (send0, recv0, cap0, bases[0], 0))

    def gather(k, out, at, cap, base):
        for j in range(cap):
            node = req_s[k, 0, base + j]
            pair = fsp[pl.ds(node, 2, stride=gap), :]
            out[at * cap + j] = pair.astype(BF16)

    def start_send(k, out, into, cap, h):
        t = asker_s[0, k]
        pltpu.make_async_remote_copy(
            src_ref=out.at[pl.ds(k * cap, cap)], dst_ref=into.at[pl.ds(me * cap, cap)],
            send_sem=ssem.at[h], recv_sem=rsem.at[h], device_id=t, device_id_type=LOGICAL,
        ).start()

    def serve(first, last, out, into, cap, base, h):
        def one(k, _):
            gather(k, out, k, cap, base)
            start_send(k - 1, out, into, cap, h)
            return 0

        gather(first, out, first, cap, base)
        lax.fori_loop(first + 1, last, one, 0)
        start_send(last - 1, out, into, cap, h)

    def serve_back(first, last, out, into, cap, base, h):
        def one(i, _):
            k = last - 1 - i
            gather(k, out, k, cap, base)
            start_send(k + 1, out, into, cap, h)
            return 0

        gather(last - 1, out, last - 1, cap, base)
        lax.fori_loop(1, last - first, one, 0)
        start_send(first, out, into, cap, h)

    out, into, cap, base, h = hops[0]
    serve(1, close, *hops[0])
    asked(close, n, 1)
    for copy in slot_copies:
        copy.start()
    serve(close, n, *hops[0])
    gather(0, into, me, cap, base)
    for out, into, cap, base, h in hops[1:]:
        serve(1, n, out, into, cap, base, h)
        gather(0, into, me, cap, base)

    for copy in index_copies[6:]:
        copy.wait()

    def relation_columns(rel_ref, out, blocks):
        def block(b, _):
            at = pl.multiple_of(b * LANES, LANES)
            row = rel_ref[:, pl.ds(at, LANES)].astype(F32)
            out[pl.ds(at, LANES), :] = jnp.broadcast_to(row, (LANES, LANES)).T
            return 0

        lax.fori_loop(0, blocks, block, 0)

    relation_columns(rel2, relc2, n_two // LANES)

    def seed_picks(b, _):
        at = pl.multiple_of(b * LANES, LANES)
        rel = rel1[:, pl.ds(at, LANES)]
        shape = (LANES // FAN1, LANES)
        first = lax.broadcasted_iota(jnp.int32, shape, 0) * FAN1
        ahead = lax.broadcasted_iota(jnp.int32, shape, 1) - first
        mine = (ahead >= 0) & (ahead < FAN1)
        pick = jnp.concatenate(
            [jnp.where(mine & (rel == r), 1.0, 0.0) for r in range(R)], axis=0
        ).astype(BF16)
        pick1[pl.ds(at, LANES), :] = pick
        tally = jnp.dot(pick, jnp.ones((LANES, LANES), BF16), preferred_element_type=F32)
        share1[pl.ds(at, LANES), :] = jnp.where(
            tally == 4.0, 0.25, jnp.where(tally == 3.0, 1.0 / 3.0, jnp.where(tally == 2.0, 0.5, 1.0))
        )
        return 0

    lax.fori_loop(0, n_one // LANES, seed_picks, 0)
    for copy in slot_copies:
        copy.wait()
    for copy in w_copies:
        copy.wait()

    def unpack(slot_s, came, out, total):
        batch = 32

        def some(b, _):
            for j in range(batch):
                i = b * batch + j
                pair = came[slot_s[0, i]].astype(F32)
                out[pl.ds(pl.multiple_of(i * 2, 2), 2), :] = pair
            return 0

        lax.fori_loop(0, total // batch, some, 0)

    def arrived(h, came, cap):
        got = came.at[pl.ds(0, (n - 1) * cap)]
        pltpu.make_async_copy(got, got, rsem.at[h]).wait()

    arrived(2, recv2, cap2)
    unpack(slot2_s, recv2, x2, n_two)
    tile = 32

    def two_means(b, _):
        f = pl.multiple_of(b * tile, tile)
        ra = relc2[pl.ds(FAN2 * f, tile, stride=FAN2), :]
        rb = relc2[pl.ds(FAN2 * f + 1, tile, stride=FAN2), :]
        share = jnp.where(ra == rb, 0.5, 1.0)
        for half in range(2):
            a = x2[pl.ds(4 * f + half, tile, stride=4), :] * share
            v = x2[pl.ds(4 * f + 2 + half, tile, stride=4), :] * share
            for r in range(R):
                mean = jnp.where(ra == r, a, 0.0) + jnp.where(rb == r, v, 0.0)
                at = r * width + half * LANES
                min1[pl.ds(f, tile), at : at + LANES] = mean.astype(BF16)
        return 0

    lax.fori_loop(0, n_one // tile, two_means, 0)

    def mean_part(b, _):
        f = pl.multiple_of(b * rows, rows)
        pre1[pl.ds(f, rows), :] = jnp.dot(
            min1[pl.ds(f, rows), :], wf[width:, :], preferred_element_type=F32
        )
        return 0

    rows = 128
    lax.fori_loop(0, n_one // rows, mean_part, 0, unroll=3)

    arrived(1, recv1, cap1)
    unpack(slot1_s, recv1, x1, n_one)

    def first_layer(b, _):
        f = pl.multiple_of(b * rows, rows)
        own = jnp.concatenate(
            [x1[pl.ds(2 * f, rows, stride=2), :], x1[pl.ds(2 * f + 1, rows, stride=2), :]], axis=1
        ).astype(BF16)
        total = jnp.dot(own, wf[:width, :], preferred_element_type=F32)
        total = total + pre1[pl.ds(f, rows), :]
        out = jnp.maximum(total, 0.0).astype(BF16)
        pick = pick1[pl.ds(f, rows), :]
        share = share1[pl.ds(f, rows), :]
        s = pl.multiple_of(b * tile, tile)
        for values, means in ((own, min0x), (out, min0h)):
            sums = jnp.dot(pick, values, preferred_element_type=F32)
            for r in range(R):
                for at in range(0, width, LANES):
                    mean = sums[r * tile : (r + 1) * tile, at : at + LANES] * share[r * tile : (r + 1) * tile]
                    means[pl.ds(s, tile), r * width + at : r * width + at + LANES] = mean.astype(BF16)
        return 0

    lax.fori_loop(0, n_one // rows, first_layer, 0, unroll=3)

    seed_part = jnp.dot(min0x[...], wf[width:, :], preferred_element_type=F32)
    second_part = jnp.dot(min0h[...], ws[width:, :], preferred_element_type=F32)

    arrived(0, recv0, cap0)
    unpack(slot0_s, recv0, x0, n_seed)
    own = jnp.concatenate(
        [x0[pl.ds(0, n_seed, stride=2), :], x0[pl.ds(1, n_seed, stride=2), :]], axis=1
    ).astype(BF16)
    h1s = jnp.maximum(
        jnp.dot(own, wf[:width, :], preferred_element_type=F32) + seed_part, 0.0
    ).astype(BF16)
    second = jnp.dot(h1s, ws[:width, :], preferred_element_type=F32) + second_part

    edges = mask_ref.shape[1]
    sources = second[:edges]
    products = sources * second[edges : 2 * edges]
    positive = lax.dot_general(
        jnp.ones((8, width), F32), products, NT,
        precision=lax.Precision.HIGHEST, preferred_element_type=F32,
    )[:1]
    negative = lax.dot_general(
        second[2 * edges :], sources, NT,
        precision=lax.Precision.HIGHEST, preferred_element_type=F32,
    )
    top = jnp.maximum(jnp.max(negative, axis=0, keepdims=True), positive)
    spread = jnp.sum(jnp.exp(negative - top), axis=0, keepdims=True) + jnp.exp(positive - top)
    edge_loss = top + jnp.log(spread) - positive
    result_ref[0:1, :] = edge_loss
    weights = mask_ref[...].astype(F32)
    left = lax.broadcasted_iota(jnp.int32, weights.shape, 1) < LANES // 2
    masked = weights * edge_loss
    both = jnp.where(
        left, masked + pltpu.roll(masked, LANES // 2, 1), weights + pltpu.roll(weights, LANES // 2, 1)
    )
    part_out[...] = both
    part_in[me] = both
    for t in peers[:0:-1]:
        pltpu.make_async_remote_copy(
            src_ref=part_out, dst_ref=part_in.at[me], send_sem=psend, recv_sem=precv,
            device_id=t, device_id_type=LOGICAL,
        ).start()
    told = part_in.at[rest]
    pltpu.make_async_copy(told, told, precv).wait()
    total = jnp.sum(part_in[...], axis=0)
    loss_sum = jnp.sum(jnp.where(left, total, 0.0), axis=1, keepdims=True)
    tally = jnp.sum(jnp.where(left, 0.0, total), axis=1, keepdims=True)
    result_ref[1:2, :] = jnp.broadcast_to(loss_sum / jnp.maximum(tally, 1.0), (1, LANES))
    pltpu.make_async_copy(told, told, psend).wait()
    sent = req_out.at[rest]
    pltpu.make_async_copy(sent, sent, qsend).wait()
    for out, _, cap, _, h in hops:
        sent = out.at[pl.ds(0, (n - 1) * cap)]
        pltpu.make_async_copy(sent, sent, ssem.at[h]).wait()


def solution(mesh):
    n = mesh.shape["dom"]

    def shards(
        features, w_first, w_second, seed_owner, seed_row, hop1_owner, hop1_row, hop1_rel,
        hop2_owner, hop2_row, hop2_rel, edge_mask,
    ):
        nodes, width = features.shape
        n_seed, n_one, n_two = seed_row.shape[0], hop1_row.shape[0], hop2_row.shape[0]
        edges = edge_mask.shape[0]
        caps = tuple(-(-2 * m // n) for m in (n_seed, n_one, n_two))
        cap0, cap1, cap2 = caps
        padded = -(-n_seed // LANES) * LANES
        vmem, hbm = pl.BlockSpec(memory_space=pltpu.VMEM), pl.BlockSpec(memory_space=pl.ANY)
        dma = pltpu.SemaphoreType.DMA

        def rows_of(cap):
            return pltpu.VMEM((n * cap, 2, LANES), BF16)

        def line(m):
            return pltpu.VMEM((1, m), jnp.int32)

        scratch = [
            line(n_seed), line(n_seed), line(n_one), line(n_one), line(n_one),
            line(n_two), line(n_two), line(n_two), line(edges),
            pltpu.VMEM((nodes, width), BF16),
            pltpu.VMEM((2 * nodes + 8, LANES), F32),
            pltpu.VMEM(w_first.shape, BF16),
            pltpu.VMEM(w_second.shape, BF16),
            pltpu.VMEM((1, padded), jnp.int32),
            pltpu.VMEM((1, padded), jnp.int32),
            pltpu.VMEM((1, padded), jnp.int32),
            pltpu.VMEM((1, n_one), jnp.int32),
            pltpu.VMEM((1, n_two), jnp.int32),
            pltpu.VMEM((n, 1, LANES), jnp.int32),
            pltpu.VMEM((n, 1, LANES), jnp.int32),
            rows_of(cap0), rows_of(cap1), rows_of(cap2),
            rows_of(cap0), rows_of(cap1), rows_of(cap2),
            pltpu.VMEM((2 * n_seed, LANES), F32),
            pltpu.VMEM((2 * n_one, LANES), F32),
            pltpu.VMEM((2 * n_two, LANES), F32),
            pltpu.VMEM((n_one, R * width), BF16),
            pltpu.VMEM((n_seed, R * width), BF16),
            pltpu.VMEM((n_seed, R * width), BF16),
            pltpu.VMEM((n_one, width), F32),
            pltpu.VMEM((n_one, LANES), BF16),
            pltpu.VMEM((n_one, LANES), F32),
            pltpu.VMEM((n_two, LANES), F32),
            pltpu.VMEM((1, edges), F32),
            pltpu.VMEM((n, 1, edges), F32),
            pltpu.SMEM((n, 1, LANES), jnp.int32),
            pltpu.SMEM((1, n), jnp.int32),
            pltpu.SMEM((1, padded), jnp.int32),
            pltpu.SMEM((1, n_one), jnp.int32),
            pltpu.SMEM((1, n_two), jnp.int32),
            dma((9,)), dma((4,)), dma((2,)), dma, dma((2,)), dma((3,)), dma((3,)), dma((5,)), dma, dma,
        ]
        result = pl.pallas_call(
            functools.partial(kernel, n, (n_seed, n_one, n_two), caps),
            out_shape=jax.ShapeDtypeStruct((2, LANES), F32),
            in_specs=[hbm] * 12,
            out_specs=vmem,
            scratch_shapes=scratch,
            compiler_params=pltpu.CompilerParams(
                collective_id=0, has_side_effects=True, vmem_limit_bytes=62 * 2**20
            ),
            name="fetch_and_score",
        )(
            features, w_first, w_second,
            seed_owner.reshape(1, n_seed), seed_row,
            hop1_owner.reshape(1, n_one), hop1_row, hop1_rel,
            hop2_owner.reshape(1, n_two), hop2_row, hop2_rel, edge_mask,
        )
        return result[0], result[1, 0]

    dom = P("dom")
    tall = P("dom", None)
    return jax.shard_map(
        shards,
        mesh=mesh,
        in_specs=(tall, P(), P(), tall, dom, tall, dom, dom, tall, dom, dom, dom),
        out_specs=(dom, P()),
        check_vma=False,
    )
```
